256 devices in a mesh: rows: 128 (over y_lo, x, z, core), feat: 2 (over y_hi).
Axes of the slice: x: 4, y: 4 (y_hi: 2, y_lo: 2; y = y_hi * 2 + y_lo), z: 8, core: 2. Of those that a mesh axis runs over, the one named last changes fastest.
Arguments:
- train_cells: bfloat16 [8192, 1536], P('rows', 'feat'), may hold values from -24 to 24
- test_cells: bfloat16 [4096, 1536], P('rows', 'feat'), may hold values from -24 to 24
- feat_weights: bfloat16 [4, 192, 192], replicated
- row_weights: bfloat16 [4, 192, 192], replicated
- mlp_up: bfloat16 [192, 768], replicated, may hold values from -0.4375 to 0.4375
- mlp_down: bfloat16 [768, 192], replicated, may hold values from -0.21875 to 0.21875
Outputs:
- train_out: bfloat16 [8192, 1536], P('rows', 'feat')
- test_out: bfloat16 [4096, 1536], P('rows', 'feat')
The draws below stay inside these ranges and needn't reach their ends.
All inputs are finite; a program needn't handle non-finite values.
Results may differ from the reference program's by a relative error of at most 0.017.
Values may be sent and summed in bfloat16 or wider, within the bound.
No kernel may reach another device: no remote copies, remote signals or barrier semaphores. Data moves between devices by JAX's collectives and lax.ppermute only.
A program may use at most 128 MiB of HBM per device.

```python
import math
import jax
import jax.numpy as jnp
from jax import lax

E = 192
HEADS = 6
HD = 32
HID = 768
F = 8
TRAIN = 8192
TEST = 4096


def attention_weights(key, query_gain):
    split_keys = jax.random.split(key, 4)
    spread = E ** (-0.5)
    query_w = jax.random.normal(split_keys[0], (E, E), jnp.float32) * query_gain * spread
    key_w = jax.random.normal(split_keys[1], (E, E), jnp.float32) * spread
    value_w = jax.random.normal(split_keys[2], (E, E), jnp.float32) * spread
    output_w = jax.random.normal(split_keys[3], (E, E), jnp.float32) * spread
    return jnp.stack([query_w, key_w, value_w, output_w]).astype(jnp.bfloat16)


def draw_feat_weights(key, part):
    return attention_weights(jax.random.fold_in(key, 3), 1.5)


def draw_row_weights(key, part):
    return attention_weights(jax.random.fold_in(key, 5), 2.5)


def train_table(key):
    key_base = jax.random.fold_in(key, 0)
    table = jax.random.normal(key_base, (TRAIN, F, E), jnp.float32)
    return jnp.clip(table, -24.0, 24.0)


def draw_train_cells(key, part):
    return train_table(jax.random.fold_in(key, 11)).reshape(TRAIN, F * E).astype(jnp.bfloat16)


def draw_test_cells(key, part):
    fresh = jax.random.normal(jax.random.fold_in(key, 13), (TEST, F, E), jnp.float32)
    return jnp.clip(fresh, -24.0, 24.0).reshape(TEST, F * E).astype(jnp.bfloat16)


def bell_draw(key, dims, scale, limit, kind=jnp.bfloat16):
    values = scale * jax.random.normal(key, dims, jnp.float32)
    return jnp.clip(values, min=-limit, max=limit).astype(kind)


def setup_inputs(seed: int = 0) -> dict:
    key_list = jax.random.split(jax.random.key(seed), 7)
    train_cells = draw_train_cells(jax.random.fold_in(key_list[6], 71), 0)
    test_cells = draw_test_cells(jax.random.fold_in(key_list[6], 71), 0)
    feat_weights = draw_feat_weights(jax.random.fold_in(key_list[6], 71), 0)
    row_weights = draw_row_weights(jax.random.fold_in(key_list[6], 71), 0)
    mlp_up = bell_draw(key_list[4], (E, HID), E ** -0.5, 0.4375)
    mlp_down = bell_draw(key_list[5], (HID, E), HID ** -0.5, 0.21875)
    return dict(train_cells=train_cells, test_cells=test_cells, feat_weights=feat_weights, row_weights=row_weights, mlp_up=mlp_up, mlp_down=mlp_down)


eps_norm = 1e-05

def layer_norm(values_in):
    centred = values_in - lax.optimization_barrier(jnp.mean(values_in, axis=-1, keepdims=True))
    spread = lax.optimization_barrier(jnp.mean(centred * centred, axis=-1, keepdims=True))
    return centred * lax.rsqrt(spread + eps_norm)

def project(normed, weight):
    return jnp.dot(normed.reshape(-1, E), weight, preferred_element_type=jnp.float32)

def round_back(values_in):
    return lax.optimization_barrier(values_in.astype(jnp.bfloat16)).astype(jnp.float32)

def feature_attention(queries, key_heads, value_heads):
    scores = jnp.einsum('rqhd,rkhd->rhqk', queries.astype(jnp.float32), key_heads.astype(jnp.float32)) * HD ** (-0.5)
    row_peak = lax.optimization_barrier(jnp.max(scores, axis=-1, keepdims=True))
    weights = jnp.exp(scores - row_peak)
    totals = lax.optimization_barrier(jnp.sum(weights, axis=-1))
    mixture = jnp.einsum('rhqk,rkhd->rqhd', round_back(weights), value_heads.astype(jnp.float32))
    return (mixture / jnp.transpose(totals, (0, 2, 1))[..., None]).astype(jnp.bfloat16)

def row_attention(queries, key_heads, value_heads):
    total_rows = queries.shape[0]
    block_rows = math.gcd(total_rows, 1024)
    query_feat = jnp.transpose(queries, (1, 0, 2, 3)).reshape(F, total_rows // block_rows, block_rows, HEADS, HD)
    key_feat = jnp.transpose(key_heads, (1, 0, 2, 3))
    value_feat = jnp.transpose(value_heads, (1, 0, 2, 3))

    def one_feature(inputs):
        query_blocks, key_one, value_one = inputs
        key_float = key_one.astype(jnp.float32)
        value_float = value_one.astype(jnp.float32)

        def one_block(query_block):
            scores = jnp.einsum('qhd,khd->hqk', query_block.astype(jnp.float32), key_float) * HD ** (-0.5)
            row_peak = lax.optimization_barrier(jnp.max(scores, axis=-1, keepdims=True))
            weights = jnp.exp(scores - row_peak)
            totals = lax.optimization_barrier(jnp.sum(weights, axis=-1))
            mixture = jnp.einsum('hqk,khd->qhd', round_back(weights), value_float)
            return (mixture / jnp.transpose(totals)[..., None]).astype(jnp.bfloat16)
        return lax.map(one_block, query_blocks).reshape(total_rows, HEADS, HD)
    mixture = lax.map(one_feature, (query_feat, key_feat, value_feat))
    return jnp.transpose(mixture, (1, 0, 2, 3))

def reference(train_cells, test_cells, feat_weights, row_weights, mlp_up, mlp_down):
    joined = jnp.concatenate([train_cells, test_cells], axis=0)
    height = joined.shape[0]
    start_cells = joined.astype(jnp.float32).reshape(height, F, E)
    normed_one = layer_norm(start_cells).astype(jnp.bfloat16)
    feat_query = project(normed_one, feat_weights[0]).astype(jnp.bfloat16).reshape(height, F, HEADS, HD)
    feat_key = project(normed_one, feat_weights[1]).astype(jnp.bfloat16).reshape(height, F, HEADS, HD)
    feat_value = project(normed_one, feat_weights[2]).astype(jnp.bfloat16).reshape(height, F, HEADS, HD)
    feat_mix = feature_attention(feat_query, feat_key, feat_value)
    feat_out = project(feat_mix, feat_weights[3]).astype(jnp.bfloat16).reshape(height, F, E)
    after_feat = start_cells + feat_out.astype(jnp.float32)
    normed_two = layer_norm(after_feat).astype(jnp.bfloat16)
    row_query = project(normed_two, row_weights[0]).astype(jnp.bfloat16).reshape(height, F, HEADS, HD)
    train_normed = normed_two[:TRAIN]
    row_key = project(train_normed, row_weights[1]).astype(jnp.bfloat16).reshape(TRAIN, F, HEADS, HD)
    row_value = project(train_normed, row_weights[2]).astype(jnp.bfloat16).reshape(TRAIN, F, HEADS, HD)
    row_mix = row_attention(row_query, row_key, row_value)
    after_row = after_feat + project(row_mix, row_weights[3]).reshape(height, F, E)
    normed_three = layer_norm(after_row).astype(jnp.bfloat16)
    hidden = jax.nn.gelu(jnp.dot(normed_three.reshape(-1, E), mlp_up, preferred_element_type=jnp.float32), approximate=False).astype(jnp.bfloat16)
    lowered = jnp.dot(hidden, mlp_down, preferred_element_type=jnp.float32).reshape(height, F, E)
    result = (after_row + lowered).astype(jnp.bfloat16).reshape(height, F * E)
    return (result[:TRAIN], result[TRAIN:])
```

```python
import math

import jax
import jax.numpy as jnp
from jax import lax
from jax.experimental import pallas as pl
from jax.experimental.pallas import tpu as pltpu
from jax.sharding import Mesh
from jax.sharding import PartitionSpec as P

E = 192
HEADS = 6
HD = 32
HID = 768
GROUPS = 4
FEATS = 8
TRAIN_ROWS = 64
TEST_ROWS = 32
ROWS = TRAIN_ROWS + TEST_ROWS
RANKS = 4
TEST_PIECE = TEST_ROWS // RANKS
TRAIN_PIECE = TRAIN_ROWS // RANKS
ASK = TEST_PIECE + TRAIN_PIECE
PIECE = TEST_PIECE + TRAIN_ROWS
PEERS = GROUPS * RANKS
OWN_Q = PEERS * ASK
ALL_Q = 2 * OWN_Q
KEYS = PEERS * TRAIN_ROWS
KEY_STEP = 256
SUMS = HD + 16
PACKED = HD + 8

eps_norm = 1e-05
log2_scale = HD ** (-0.5) * math.log2(math.e)


bf16 = jnp.bfloat16
f32 = jnp.float32


def mm(left, right):
    return jnp.dot(left, right, preferred_element_type=f32)


def mm_nt(left, right):
    return lax.dot_general(left, right, (((1,), (1,)), ((), ())), preferred_element_type=f32)


def layer_norm(values_in):
    centred = values_in - jnp.mean(values_in, axis=-1, keepdims=True)
    spread = jnp.mean(centred * centred, axis=-1, keepdims=True)
    return centred * lax.rsqrt(spread + eps_norm)


def call(kernel, outs, args, name, flops, scratch=(), limit=40):
    in_vmem = pl.BlockSpec(memory_space=pltpu.VMEM)
    return pl.pallas_call(
        kernel,
        out_shape=outs,
        in_specs=[in_vmem] * len(args),
        out_specs=[in_vmem] * len(outs),
        scratch_shapes=list(scratch),
        compiler_params=pltpu.CompilerParams(vmem_limit_bytes=limit * 2**20),
        cost_estimate=pl.CostEstimate(flops=flops, transcendentals=0, bytes_accessed=2**20),
        name=name,
    )(*args)


def before_kernel(train_ref, test_ref, other_ref, weights_ref, after_ref, send_ref):
    def cell(index):
        left = (index % GROUPS) * E
        if index < GROUPS:
            parts = [train_ref[:, left : left + E], test_ref[:, left : left + E]]
            return jnp.concatenate([part.astype(f32) for part in parts], axis=0)
        return other_ref[:, left : left + E].astype(f32)

    cells = [cell(index) for index in range(FEATS)]
    normed = jnp.concatenate([layer_norm(one).astype(bf16) for one in cells], axis=0)
    queries = (mm(normed[: GROUPS * ROWS], weights_ref[0]) * log2_scale).astype(bf16)
    keys = mm(normed, weights_ref[1]).astype(bf16)
    values = mm(normed, weights_ref[2])
    values = values.astype(bf16).astype(f32)
    head_of = lax.broadcasted_iota(jnp.int32, (E, 128), 0) >> 5
    gather = jnp.where(head_of == lax.broadcasted_iota(jnp.int32, (E, 128), 1), 1.0, 0.0).astype(bf16)
    head_to = lax.broadcasted_iota(jnp.int32, (128, E), 1) >> 5
    spread = jnp.where(head_to == lax.broadcasted_iota(jnp.int32, (128, E), 0), 1.0, 0.0).astype(bf16)
    mixtures = []
    for index in range(GROUPS):
        asked = queries[index * ROWS : (index + 1) * ROWS]
        products = jnp.concatenate(
            [asked * keys[j * ROWS : (j + 1) * ROWS] for j in range(FEATS)], axis=0
        )
        scores = mm(products, gather)
        pieces = [scores[j * ROWS : (j + 1) * ROWS] for j in range(FEATS)]
        peak = pieces[0]
        for one in pieces[1:]:
            peak = jnp.maximum(peak, one)
        weights = [jnp.exp2(one - peak) for one in pieces]
        total = weights[0]
        for one in weights[1:]:
            total = total + one
        high = total.astype(bf16)
        low = (total - high.astype(f32)).astype(bf16)
        wide = mm(jnp.concatenate([one.astype(bf16) for one in weights] + [high, low], axis=0), spread)
        mixed = wide[:ROWS] * values[:ROWS]
        for j in range(1, FEATS):
            mixed = mixed + wide[j * ROWS : (j + 1) * ROWS] * values[j * ROWS : (j + 1) * ROWS]
        whole = wide[FEATS * ROWS : (FEATS + 1) * ROWS] + wide[(FEATS + 1) * ROWS :]
        mixtures.append((mixed / whole).astype(bf16))
    moved = mm(jnp.concatenate(mixtures, axis=0), weights_ref[3]).astype(bf16).astype(f32)
    for index in range(GROUPS):
        after = cells[index] + moved[index * ROWS : (index + 1) * ROWS]
        after_ref[index] = after
        second = layer_norm(after)
        for rank in range(RANKS):
            turn = rank * TRAIN_PIECE
            at = TRAIN_ROWS + rank * TEST_PIECE
            parts = [second[at : at + TEST_PIECE], second[turn:TRAIN_ROWS]]
            if turn:
                parts.append(second[:turn])
            send_ref[index * RANKS + rank] = jnp.concatenate(parts, axis=0).astype(bf16)


def attend_kernel(first, last, refs):
    refs = list(refs)
    if first:
        ask_ref, other_ref, keys_ref, wq_ref, wk_ref, wv_ref = refs[:6]
        folded_ref, peak_out, mix_out = refs[6:9]
        scratch = refs[9:]
    else:
        keys_ref, wv_ref, folded_ref, peak_in, mix_in = refs[:5]
        if last:
            stay_out, leave_out = refs[5:7]
        else:
            peak_out, mix_out = refs[5:7]
        scratch = refs[7:]
    values_ref, even_ref, odd_ref = scratch
    if first:
        asked = jnp.concatenate([ask_ref[...], other_ref[...]], axis=0)
        queries = (mm(asked, wq_ref[...]) * log2_scale).astype(bf16)
        for head in range(HEADS):
            part = slice(head * HD, (head + 1) * HD)
            folded_ref[head] = mm_nt(wk_ref[:, part], queries[:, part]).astype(bf16)
    values = mm_nt(wv_ref[...], keys_ref[...]).astype(bf16)
    for head in range(HEADS):
        values_ref[head, 0:HD, :] = values[head * HD : (head + 1) * HD, :]
        values_ref[head, HD:SUMS, :] = jnp.ones((SUMS - HD, KEYS), bf16)

    def scores(head, into_ref):
        peak = None
        for step in range(KEYS // KEY_STEP):
            span = slice(step * KEY_STEP, (step + 1) * KEY_STEP)
            block = mm(keys_ref[span, :], folded_ref[head])
            into_ref[span, :] = block
            top = jnp.max(block.reshape(KEY_STEP // 8, 8, ALL_Q), axis=0)
            peak = top if peak is None else jnp.maximum(peak, top)
        return jnp.max(peak, axis=0, keepdims=True)

    def mix(head, from_ref, peak):
        if not first:
            old = peak_in[head][0:1, :]
            peak = jnp.maximum(peak, old)
        weights = jnp.exp2(from_ref[...] - peak).astype(bf16)
        mixed = mm(values_ref[head], weights)
        if not first:
            mixed = mixed + mix_in[head] * jnp.exp2(old - peak)
        if last:
            joined = jnp.concatenate([mixed[: HD + 1], peak, mixed[HD + 2 : PACKED]], axis=0)
            stay_out[head] = joined[:, :OWN_Q]
            leave_out[head] = joined[:, OWN_Q:]
        else:
            mix_out[head] = mixed
            peak_out[head] = jnp.broadcast_to(peak, (8, ALL_Q))

    def step(pair, peak_even):
        head = 2 * pair
        peak_odd = scores(head + 1, odd_ref)
        mix(head, even_ref, peak_even)
        peak_next = scores(jnp.minimum(head + 2, HEADS - 1), even_ref)
        mix(head + 1, odd_ref, peak_odd)
        return peak_next

    lax.fori_loop(0, HEADS // 2, step, scores(0, even_ref))


def attend(first, last, args):
    if last:
        outs = [jax.ShapeDtypeStruct((HEADS, PACKED, OWN_Q), f32)] * 2
    else:
        outs = [
            jax.ShapeDtypeStruct((HEADS, 8, ALL_Q), f32),
            jax.ShapeDtypeStruct((HEADS, SUMS, ALL_Q), f32),
        ]
    if first:
        outs = [jax.ShapeDtypeStruct((HEADS, E, ALL_Q), bf16)] + outs
    return call(
        lambda *refs: attend_kernel(first, last, refs),
        outs,
        args,
        "attend_first" if first else "attend_last" if last else "attend_next",
        4 * HEADS * KEYS * ALL_Q * E,
        scratch=[
            pltpu.VMEM((HEADS, SUMS, KEYS), bf16),
            pltpu.VMEM((KEYS, ALL_Q), f32),
            pltpu.VMEM((KEYS, ALL_Q), f32),
        ],
        limit=48,
    )


def merge_kernel(stay_ref, came_ref, send_ref):
    parts = []
    for head in range(HEADS):
        stay = stay_ref[head]
        came = came_ref[head]
        peak = jnp.maximum(stay[HD + 1 : HD + 2], came[HD + 1 : HD + 2])
        fade_stay = jnp.exp2(stay[HD + 1 : HD + 2] - peak)
        fade_came = jnp.exp2(came[HD + 1 : HD + 2] - peak)
        total = stay[HD : HD + 1] * fade_stay + came[HD : HD + 1] * fade_came
        mixed = stay[:HD] * fade_stay + came[:HD] * fade_came
        parts.append(mixed / total)
    turned = jnp.concatenate(parts, axis=0).T
    for peer in range(PEERS):
        send_ref[peer] = turned[peer * ASK : (peer + 1) * ASK].astype(bf16)


def after_kernel(came_ref, after_ref, wo_ref, up_ref, down_ref, train_ref, test_ref):
    mixes = []
    for index in range(GROUPS):
        came = [came_ref[index * RANKS + rank].astype(f32) for rank in range(RANKS)]
        mixes += [one[TEST_PIECE:] for one in came] + [one[:TEST_PIECE] for one in came]
    row_mix = jnp.concatenate(mixes, axis=0).astype(bf16)
    after_row = after_ref[...].reshape(GROUPS * ROWS, E) + mm(row_mix, wo_ref[...])
    third = layer_norm(after_row).astype(bf16)
    raised = mm(third, up_ref[...])
    hidden = (0.5 * raised * (1.0 + lax.erf(raised * (0.5**0.5)))).astype(bf16)
    result = (after_row + mm(hidden, down_ref[...])).astype(bf16)
    for index in range(GROUPS):
        low = index * ROWS
        left = index * E
        train_ref[:, left : left + E] = result[low : low + TRAIN_ROWS]
        test_ref[:, left : left + E] = result[low + TRAIN_ROWS : low + ROWS]


def shift(size, by):
    return [(index, (index + by) % size) for index in range(size)]


def body(train_cells, test_cells, feat_weights, row_weights, mlp_up, mlp_down):
    swap = [(0, 1), (1, 0)]
    joined = jnp.concatenate([train_cells, test_cells], axis=0)
    other = lax.ppermute(joined, "feat", swap)
    after_feat, pieces = call(
        before_kernel,
        [
            jax.ShapeDtypeStruct((GROUPS, ROWS, E), f32),
            jax.ShapeDtypeStruct((PEERS, PIECE, E), bf16),
        ],
        (train_cells, test_cells, other, feat_weights),
        "before",
        10**9,
    )
    received = lax.all_to_all(
        pieces, ("y_lo", "z_lo", "z_hi"), split_axis=0, concat_axis=0, tiled=True
    )
    asked = received[:, :ASK].reshape(OWN_Q, E)
    keys = received[:, TEST_PIECE:].reshape(KEYS, E)
    asked_other = lax.ppermute(asked, "core", swap)
    distant = [lax.ppermute(keys, "x", shift(4, by)) for by in (1, 3, 2)]
    value_turned = row_weights[2].T
    folded, peak, mix = attend(
        True,
        False,
        (asked, asked_other, keys, row_weights[0], row_weights[1], value_turned),
    )
    for one in distant[:-1]:
        peak, mix = attend(False, False, (one, value_turned, folded, peak, mix))
    stay, leave = attend(False, True, (distant[-1], value_turned, folded, peak, mix))
    came = lax.ppermute(leave, "core", swap)
    mixed = call(
        merge_kernel,
        [jax.ShapeDtypeStruct((PEERS, ASK, E), bf16)],
        (stay, came),
        "merge",
        10**7,
    )[0]
    returned = lax.all_to_all(
        mixed, ("y_lo", "z_lo", "z_hi"), split_axis=0, concat_axis=0, tiled=True
    )
    train_out, test_out = call(
        after_kernel,
        [
            jax.ShapeDtypeStruct((TRAIN_ROWS, GROUPS * E), bf16),
            jax.ShapeDtypeStruct((TEST_ROWS, GROUPS * E), bf16),
        ],
        (returned, after_feat, row_weights[3], mlp_up, mlp_down),
        "after",
        10**9,
    )
    return (train_out, test_out)


def solution(mesh):
    split = Mesh(
        mesh.devices.reshape(2, 4, 4, 2, 2, 2), ("y_lo", "x", "z_hi", "z_lo", "core", "feat")
    )
    rows = ("y_lo", "x", "z_hi", "z_lo", "core")
    return jax.shard_map(
        body,
        mesh=split,
        in_specs=(P(rows, "feat"), P(rows, "feat"), P(), P(), P(), P()),
        out_specs=(P(rows, "feat"), P(rows, "feat")),
        check_vma=False,
    )
```

```python
import math

import jax
import jax.numpy as jnp
from jax import lax
from jax.experimental import pallas as pl
from jax.experimental.pallas import tpu as pltpu
from jax.sharding import Mesh
from jax.sharding import PartitionSpec as P

E = 192
HEADS = 6
HD = 32
HID = 768
GROUPS = 4
FEATS = 8
TRAIN_ROWS = 64
TEST_ROWS = 32
ROWS = TRAIN_ROWS + TEST_ROWS
SIDE = 4
LANES = 128
REST = E - LANES
TRAIN_PACK = TRAIN_ROWS + TRAIN_ROWS // 2
PACK = ROWS + ROWS // 2
OWN_Q = GROUPS * ROWS
ALL_Q = 2 * OWN_Q
SOURCES = GROUPS * SIDE
KEYS = SOURCES * TRAIN_ROWS
KEY_STEP = 256
SUMS = HD + 16
STATE = HD + 8

eps_norm = 1e-05
log2_scale = HD ** (-0.5) * math.log2(math.e)


bf16 = jnp.bfloat16
f32 = jnp.float32


def mm(left, right):
    return jnp.dot(left, right, preferred_element_type=f32)


def mm_nt(left, right):
    return lax.dot_general(left, right, (((1,), (1,)), ((), ())), preferred_element_type=f32)


def layer_norm(values_in):
    centred = values_in - jnp.mean(values_in, axis=-1, keepdims=True)
    spread = jnp.mean(centred * centred, axis=-1, keepdims=True)
    return centred * lax.rsqrt(spread + eps_norm)


def call(kernel, outs, args, name, flops, scratch=(), limit=40):
    in_vmem = pl.BlockSpec(memory_space=pltpu.VMEM)
    return pl.pallas_call(
        kernel,
        out_shape=outs,
        in_specs=[in_vmem] * len(args),
        out_specs=[in_vmem] * len(outs),
        scratch_shapes=list(scratch),
        compiler_params=pltpu.CompilerParams(vmem_limit_bytes=limit * 2**20),
        cost_estimate=pl.CostEstimate(flops=flops, transcendentals=0, bytes_accessed=2**20),
        name=name,
    )(*args)


def pack_rows(rows):
    half = rows.shape[0] // 2
    rest = rows[:, LANES:]
    return [rows[:, :LANES], jnp.concatenate([rest[:half], rest[half:]], axis=1)]


def pack(rows):
    parts = pack_rows(rows[:TRAIN_ROWS]) + pack_rows(rows[TRAIN_ROWS:])
    return jnp.concatenate(parts, axis=0).astype(bf16)


def unpack_rows(packed):
    height = packed.shape[0] * 2 // 3
    rest = packed[height:]
    rest = jnp.concatenate([rest[:, :REST], rest[:, REST:]], axis=0)
    return jnp.concatenate([packed[:height], rest], axis=1)


def unpack(packed):
    packed = packed.astype(f32)
    parts = [unpack_rows(packed[:TRAIN_PACK]), unpack_rows(packed[TRAIN_PACK:])]
    return jnp.concatenate(parts, axis=0)


def near_kernel(joined_ref, weights_ref, cells_ref, query_ref, key_ref, value_ref):
    parts = []
    for index in range(GROUPS):
        cell = joined_ref[:, index * E : (index + 1) * E].astype(f32)
        cells_ref[index] = cell
        parts.append(layer_norm(cell).astype(bf16))
    normed = jnp.concatenate(parts, axis=0)
    query_ref[...] = (mm(normed, weights_ref[0]) * log2_scale).astype(bf16)
    key_ref[...] = mm(normed, weights_ref[1]).astype(bf16)
    value_ref[...] = mm(normed, weights_ref[2]).astype(bf16)


def before_kernel(
    other_ref, weights_ref, cells_ref, query_ref, key_ref, value_ref, after_ref, send_ref
):
    parts = []
    for index in range(GROUPS):
        cell = other_ref[:, index * E : (index + 1) * E].astype(f32)
        parts.append(layer_norm(cell).astype(bf16))
    normed = jnp.concatenate(parts, axis=0)
    far_keys = mm(normed, weights_ref[1]).astype(bf16)
    far_values = mm(normed, weights_ref[2]).astype(bf16)
    queries = query_ref[...]
    keys = jnp.concatenate([key_ref[...], far_keys], axis=0)
    values = jnp.concatenate([value_ref[...], far_values], axis=0).astype(f32)
    head_of = lax.broadcasted_iota(jnp.int32, (E, 128), 0) >> 5
    gather = jnp.where(head_of == lax.broadcasted_iota(jnp.int32, (E, 128), 1), 1.0, 0.0).astype(bf16)
    head_to = lax.broadcasted_iota(jnp.int32, (128, E), 1) >> 5
    spread = jnp.where(head_to == lax.broadcasted_iota(jnp.int32, (128, E), 0), 1.0, 0.0).astype(bf16)
    mixtures = []
    for index in range(GROUPS):
        asked = queries[index * ROWS : (index + 1) * ROWS]
        products = jnp.concatenate(
            [asked * keys[j * ROWS : (j + 1) * ROWS] for j in range(FEATS)], axis=0
        )
        scores = mm(products, gather)
        pieces = [scores[j * ROWS : (j + 1) * ROWS] for j in range(FEATS)]
        peak = pieces[0]
        for one in pieces[1:]:
            peak = jnp.maximum(peak, one)
        weights = [jnp.exp2(one - peak) for one in pieces]
        total = weights[0]
        for one in weights[1:]:
            total = total + one
        high = total.astype(bf16)
        low = (total - high.astype(f32)).astype(bf16)
        wide = mm(jnp.concatenate([one.astype(bf16) for one in weights] + [high, low], axis=0), spread)
        mixed = wide[:ROWS] * values[:ROWS]
        for j in range(1, FEATS):
            mixed = mixed + wide[j * ROWS : (j + 1) * ROWS] * values[j * ROWS : (j + 1) * ROWS]
        whole = wide[FEATS * ROWS : (FEATS + 1) * ROWS] + wide[(FEATS + 1) * ROWS :]
        mixtures.append((mixed / whole).astype(bf16))
    moved = mm(jnp.concatenate(mixtures, axis=0), weights_ref[3]).astype(bf16).astype(f32)
    for index in range(GROUPS):
        after = cells_ref[index] + moved[index * ROWS : (index + 1) * ROWS]
        after_ref[index] = after
        send_ref[index] = pack(layer_norm(after))


def fold_kernel(own_ref, other_ref, weights_ref, folded_ref):
    parts = [unpack(one_ref[index]) for one_ref in (own_ref, other_ref) for index in range(GROUPS)]
    asked = jnp.concatenate(parts, axis=0).astype(bf16)
    queries = (mm(asked, weights_ref[0]) * log2_scale).astype(bf16)
    weight = weights_ref[1]
    for head in range(HEADS):
        part = slice(head * HD, (head + 1) * HD)
        folded_ref[head] = mm_nt(weight[:, part], queries[:, part]).astype(bf16)


def attend_kernel(first, last, refs):
    refs = list(refs)
    packed_ref, wv_ref, folded_ref = refs[:3]
    refs = refs[3:]
    if not first:
        peak_in, mix_in = refs[:2]
        refs = refs[2:]
    if last:
        stay_out, leave_out = refs[:2]
    else:
        peak_out, mix_out = refs[:2]
    keys_ref, values_ref, even_ref, odd_ref = refs[2:]
    half = TRAIN_ROWS // 2
    for source in range(SOURCES):
        low = source * TRAIN_ROWS
        top = source * TRAIN_PACK
        rest = packed_ref[top + TRAIN_ROWS : top + TRAIN_PACK, :]
        keys_ref[low : low + TRAIN_ROWS, :LANES] = packed_ref[top : top + TRAIN_ROWS, :]
        keys_ref[low : low + half, LANES:] = rest[:, :REST]
        keys_ref[low + half : low + TRAIN_ROWS, LANES:] = rest[:, REST:]
    values = mm_nt(wv_ref[...], keys_ref[...]).astype(bf16)
    for head in range(HEADS):
        values_ref[head, 0:HD, :] = values[head * HD : (head + 1) * HD, :]
        values_ref[head, HD:SUMS, :] = jnp.ones((SUMS - HD, KEYS), bf16)

    def scores(head, into_ref):
        peak = None
        for step in range(KEYS // KEY_STEP):
            span = slice(step * KEY_STEP, (step + 1) * KEY_STEP)
            block = mm(keys_ref[span, :], folded_ref[head])
            into_ref[span, :] = block
            top = jnp.max(block.reshape(KEY_STEP // 8, 8, ALL_Q), axis=0)
            peak = top if peak is None else jnp.maximum(peak, top)
        return jnp.max(peak, axis=0, keepdims=True)

    def mix(head, from_ref, peak):
        if not first:
            old = peak_in[head][0:1, :]
            peak = jnp.maximum(peak, old)
        weights = jnp.exp2(from_ref[...] - peak).astype(bf16)
        mixed = mm(values_ref[head], weights)
        if not first:
            mixed = mixed + mix_in[head] * jnp.exp2(old - peak)
        if last:
            joined = jnp.concatenate([mixed[: HD + 1], peak, mixed[HD + 2 : STATE]], axis=0)
            stay_out[head] = joined[:, :OWN_Q]
            leave_out[head] = joined[:, OWN_Q:]
        else:
            mix_out[head] = mixed
            peak_out[head] = jnp.broadcast_to(peak, (8, ALL_Q))

    def step(pair, peak_even):
        head = 2 * pair
        peak_odd = scores(head + 1, odd_ref)
        mix(head, even_ref, peak_even)
        peak_next = scores(jnp.minimum(head + 2, HEADS - 1), even_ref)
        mix(head + 1, odd_ref, peak_odd)
        return peak_next

    lax.fori_loop(0, HEADS // 2, step, scores(0, even_ref))


def attend(first, last, args):
    if last:
        outs = [jax.ShapeDtypeStruct((HEADS, STATE, OWN_Q), f32)] * 2
    else:
        outs = [
            jax.ShapeDtypeStruct((HEADS, 8, ALL_Q), f32),
            jax.ShapeDtypeStruct((HEADS, SUMS, ALL_Q), f32),
        ]
    return call(
        lambda *refs: attend_kernel(first, last, refs),
        outs,
        args,
        "attend_first" if first else "attend_last" if last else "attend_next",
        4 * HEADS * KEYS * ALL_Q * E,
        scratch=[
            pltpu.VMEM((KEYS, E), bf16),
            pltpu.VMEM((HEADS, SUMS, KEYS), bf16),
            pltpu.VMEM((KEYS, ALL_Q), f32),
            pltpu.VMEM((KEYS, ALL_Q), f32),
        ],
        limit=48,
    )


def merge_kernel(stay_ref, came_ref, send_ref):
    parts = []
    for head in range(HEADS):
        stay = stay_ref[head]
        came = came_ref[head]
        peak = jnp.maximum(stay[HD + 1 : HD + 2], came[HD + 1 : HD + 2])
        fade_stay = jnp.exp2(stay[HD + 1 : HD + 2] - peak)
        fade_came = jnp.exp2(came[HD + 1 : HD + 2] - peak)
        total = stay[HD : HD + 1] * fade_stay + came[HD : HD + 1] * fade_came
        mixed = stay[:HD] * fade_stay + came[:HD] * fade_came
        parts.append(mixed / total)
    turned = jnp.concatenate(parts, axis=0).T
    for peer in range(GROUPS):
        send_ref[peer] = pack(turned[peer * ROWS : (peer + 1) * ROWS])


def after_kernel(came_ref, after_ref, wo_ref, up_ref, down_ref, train_ref, test_ref):
    mixes = [unpack(came_ref[index]) for index in range(GROUPS)]
    row_mix = jnp.concatenate(mixes, axis=0).astype(bf16)
    after_row = after_ref[...].reshape(GROUPS * ROWS, E) + mm(row_mix, wo_ref[...])
    third = layer_norm(after_row).astype(bf16)
    raised = mm(third, up_ref[...])
    hidden = (0.5 * raised * (1.0 + lax.erf(raised * (0.5**0.5)))).astype(bf16)
    result = (after_row + mm(hidden, down_ref[...])).astype(bf16)
    for index in range(GROUPS):
        low = index * ROWS
        left = index * E
        train_ref[:, left : left + E] = result[low : low + TRAIN_ROWS]
        test_ref[:, left : left + E] = result[low + TRAIN_ROWS : low + ROWS]


def shift(size, by):
    return [(index, (index + by) % size) for index in range(size)]


def body(train_cells, test_cells, feat_weights, row_weights, mlp_up, mlp_down):
    swap = [(0, 1), (1, 0)]
    joined = jnp.concatenate([train_cells, test_cells], axis=0)
    other = lax.ppermute(joined, "feat", swap)
    wide = (GROUPS * ROWS, E)
    near = call(
        near_kernel,
        [jax.ShapeDtypeStruct((GROUPS, ROWS, E), f32)] + [jax.ShapeDtypeStruct(wide, bf16)] * 3,
        (joined, feat_weights),
        "near",
        10**9,
    )
    after_feat, pieces = call(
        before_kernel,
        [
            jax.ShapeDtypeStruct((GROUPS, ROWS, E), f32),
            jax.ShapeDtypeStruct((GROUPS, PACK, LANES), bf16),
        ],
        (other, feat_weights, *near),
        "before",
        10**9,
    )
    classes = ("y_lo", "z_lo")
    received = lax.all_to_all(pieces, classes, split_axis=0, concat_axis=0, tiled=True)
    keys = received[:, :TRAIN_PACK].reshape(GROUPS * TRAIN_PACK, LANES)
    column = [keys] + [lax.ppermute(keys, "z_hi", shift(SIDE, by)) for by in (1, 3, 2)]
    received_other = lax.ppermute(received, "core", swap)
    folded = call(
        fold_kernel,
        [jax.ShapeDtypeStruct((HEADS, E, ALL_Q), bf16)],
        (received, received_other, row_weights),
        "fold",
        10**9,
    )[0]
    keys = jnp.concatenate(column, axis=0)
    value_turned = row_weights[2].T
    distant = [lax.ppermute(keys, "x", shift(4, by)) for by in (1, 3)]
    peak, mix = attend(True, False, (keys, value_turned, folded))
    keys, peak, mix = lax.optimization_barrier((keys, peak, mix))
    distant.append(lax.ppermute(keys, "x", shift(4, 2)))
    for one in distant[:-1]:
        peak, mix = attend(False, False, (one, value_turned, folded, peak, mix))
    stay, leave = attend(False, True, (distant[-1], value_turned, folded, peak, mix))
    came = lax.ppermute(leave, "core", swap)
    mixed = call(
        merge_kernel,
        [jax.ShapeDtypeStruct((GROUPS, PACK, LANES), bf16)],
        (stay, came),
        "merge",
        10**7,
    )[0]
    returned = lax.all_to_all(mixed, classes, split_axis=0, concat_axis=0, tiled=True)
    train_out, test_out = call(
        after_kernel,
        [
            jax.ShapeDtypeStruct((TRAIN_ROWS, GROUPS * E), bf16),
            jax.ShapeDtypeStruct((TEST_ROWS, GROUPS * E), bf16),
        ],
        (returned, after_feat, row_weights[3], mlp_up, mlp_down),
        "after",
        10**9,
    )
    return (train_out, test_out)


def solution(mesh):
    split = Mesh(
        mesh.devices.reshape(2, 4, 4, 2, 2, 2), ("y_lo", "x", "z_hi", "z_lo", "core", "feat")
    )
    rows = ("y_lo", "x", "z_hi", "z_lo", "core")
    return jax.shard_map(
        body,
        mesh=split,
        in_specs=(P(rows, "feat"), P(rows, "feat"), P(), P(), P(), P()),
        out_specs=(P(rows, "feat"), P(rows, "feat")),
        check_vma=False,
    )
```

```python
import math

import jax
import jax.numpy as jnp
from jax import lax
from jax.experimental import pallas as pl
from jax.experimental.pallas import tpu as pltpu
from jax.sharding import Mesh
from jax.sharding import PartitionSpec as P

E = 192
HEADS = 6
HD = 32
HID = 768
GROUPS = 4
FEATS = 8
TRAIN_ROWS = 64
TEST_ROWS = 32
ROWS = TRAIN_ROWS + TEST_ROWS
SIDE = 4
LANES = 128
REST = E - LANES
TRAIN_PACK = TRAIN_ROWS + TRAIN_ROWS // 2
PACK = ROWS + ROWS // 2
OWN_Q = GROUPS * ROWS
ALL_Q = 2 * OWN_Q
SOURCES = GROUPS * SIDE
KEYS = SOURCES * TRAIN_ROWS
SUMS = HD + 16
FOLD = E + 16
PROBES = 64
HEADS_STEP = 3
STATE = HD + 8

eps_norm = 1e-05
far_below = -3e38
safe_size = 2.0**60
log2_scale = HD ** (-0.5) * math.log2(math.e)


bf16 = jnp.bfloat16
f32 = jnp.float32


def mm(left, right):
    return jnp.dot(left, right, preferred_element_type=f32)


def mm_nt(left, right):
    return lax.dot_general(left, right, (((1,), (1,)), ((), ())), preferred_element_type=f32)


def layer_norm(values_in):
    centred = values_in - jnp.mean(values_in, axis=-1, keepdims=True)
    spread = jnp.mean(centred * centred, axis=-1, keepdims=True)
    return centred * lax.rsqrt(spread + eps_norm)


def call(kernel, outs, args, name, flops, scratch=(), limit=40):
    in_vmem = pl.BlockSpec(memory_space=pltpu.VMEM)
    return pl.pallas_call(
        kernel,
        out_shape=outs,
        in_specs=[in_vmem] * len(args),
        out_specs=[in_vmem] * len(outs),
        scratch_shapes=list(scratch),
        compiler_params=pltpu.CompilerParams(vmem_limit_bytes=limit * 2**20),
        cost_estimate=pl.CostEstimate(flops=flops, transcendentals=0, bytes_accessed=2**20),
        name=name,
    )(*args)


def pack_rows(rows):
    half = rows.shape[0] // 2
    rest = rows[:, LANES:]
    return [rows[:, :LANES], jnp.concatenate([rest[:half], rest[half:]], axis=1)]


def pack(rows):
    parts = pack_rows(rows[:TRAIN_ROWS]) + pack_rows(rows[TRAIN_ROWS:])
    return jnp.concatenate(parts, axis=0).astype(bf16)


def unpack_rows(packed):
    height = packed.shape[0] * 2 // 3
    rest = packed[height:]
    rest = jnp.concatenate([rest[:, :REST], rest[:, REST:]], axis=0)
    return jnp.concatenate([packed[:height], rest], axis=1)


def unpack(packed):
    packed = packed.astype(f32)
    parts = [unpack_rows(packed[:TRAIN_PACK]), unpack_rows(packed[TRAIN_PACK:])]
    return jnp.concatenate(parts, axis=0)


def near_kernel(train_ref, test_ref, weights_ref, cells_ref, query_ref, key_ref, value_ref):
    parts = []
    for index in range(GROUPS):
        span = slice(index * E, (index + 1) * E)
        cell = [one_ref[:, span].astype(f32) for one_ref in (train_ref, test_ref)]
        cell = jnp.concatenate(cell, axis=0)
        cells_ref[index] = cell
        parts.append(layer_norm(cell).astype(bf16))
    normed = jnp.concatenate(parts, axis=0)
    query_ref[...] = (mm(normed, weights_ref[0]) * log2_scale).astype(bf16)
    key_ref[...] = mm(normed, weights_ref[1]).astype(bf16)
    value_ref[...] = mm(normed, weights_ref[2]).astype(bf16)


def before_kernel(
    other_ref, weights_ref, cells_ref, query_ref, key_ref, value_ref, after_ref, send_ref
):
    parts = []
    for index in range(GROUPS):
        cell = other_ref[:, index * E : (index + 1) * E].astype(f32)
        parts.append(layer_norm(cell).astype(bf16))
    normed = jnp.concatenate(parts, axis=0)
    far_keys = mm(normed, weights_ref[1]).astype(bf16)
    far_values = mm(normed, weights_ref[2]).astype(bf16)
    queries = query_ref[...]
    keys = jnp.concatenate([key_ref[...], far_keys], axis=0)
    values = jnp.concatenate([value_ref[...], far_values], axis=0).astype(f32)
    head_of = lax.broadcasted_iota(jnp.int32, (E, 128), 0) >> 5
    gather = jnp.where(head_of == lax.broadcasted_iota(jnp.int32, (E, 128), 1), 1.0, 0.0).astype(bf16)
    head_to = lax.broadcasted_iota(jnp.int32, (128, E), 1) >> 5
    spread = jnp.where(head_to == lax.broadcasted_iota(jnp.int32, (128, E), 0), 1.0, 0.0).astype(bf16)
    mixtures = []
    for index in range(GROUPS):
        asked = queries[index * ROWS : (index + 1) * ROWS]
        products = jnp.concatenate(
            [asked * keys[j * ROWS : (j + 1) * ROWS] for j in range(FEATS)], axis=0
        )
        scores = mm(products, gather)
        pieces = [scores[j * ROWS : (j + 1) * ROWS] for j in range(FEATS)]
        peak = pieces[0]
        for one in pieces[1:]:
            peak = jnp.maximum(peak, one)
        weights = [jnp.exp2(one - peak) for one in pieces]
        total = weights[0]
        for one in weights[1:]:
            total = total + one
        high = total.astype(bf16)
        low = (total - high.astype(f32)).astype(bf16)
        wide = mm(jnp.concatenate([one.astype(bf16) for one in weights] + [high, low], axis=0), spread)
        mixed = wide[:ROWS] * values[:ROWS]
        for j in range(1, FEATS):
            mixed = mixed + wide[j * ROWS : (j + 1) * ROWS] * values[j * ROWS : (j + 1) * ROWS]
        whole = wide[FEATS * ROWS : (FEATS + 1) * ROWS] + wide[(FEATS + 1) * ROWS :]
        mixtures.append((mixed / whole).astype(bf16))
    moved = mm(jnp.concatenate(mixtures, axis=0), weights_ref[3]).astype(bf16).astype(f32)
    for index in range(GROUPS):
        after = cells_ref[index] + moved[index * ROWS : (index + 1) * ROWS]
        after_ref[index] = after
        send_ref[index] = pack(layer_norm(after))


def fold_kernel(own_ref, other_ref, weights_ref, folded_ref):
    parts = [unpack(one_ref[index]) for one_ref in (own_ref, other_ref) for index in range(GROUPS)]
    asked = jnp.concatenate(parts, axis=0).astype(bf16)
    probes = jnp.concatenate([parts[0][:PROBES], parts[GROUPS][:PROBES]], axis=0).astype(bf16)
    queries = (mm(asked, weights_ref[0]) * log2_scale).astype(bf16)
    weight = weights_ref[1]
    row = lax.broadcasted_iota(jnp.int32, (FOLD - E, ALL_Q), 0)
    for head in range(HEADS):
        part = slice(head * HD, (head + 1) * HD)
        folded = mm_nt(weight[:, part], queries[:, part]).astype(bf16)
        peak = jnp.max(mm(probes, folded), axis=0, keepdims=True)
        folded_ref[head, :E, :] = folded
        folded_ref[head, E:, :] = jnp.where(row == 0, -peak, 0.0).astype(bf16)


def unpack_keys(packed_ref, keys_ref):
    half = TRAIN_ROWS // 2
    for source in range(SOURCES):
        low = source * TRAIN_ROWS
        top = source * TRAIN_PACK
        rest = packed_ref[top + TRAIN_ROWS : top + TRAIN_PACK, :]
        keys_ref[low : low + TRAIN_ROWS, :LANES] = packed_ref[top : top + TRAIN_ROWS, :]
        keys_ref[low : low + half, LANES:E] = rest[:, :REST]
        keys_ref[low + half : low + TRAIN_ROWS, LANES:E] = rest[:, REST:]
    keys_ref[:, E:] = jnp.ones((KEYS, FOLD - E), bf16)


def turn_values(wv_ref, keys_ref, values_ref):
    values = mm_nt(wv_ref[...], keys_ref[:, :E]).astype(bf16)
    for head in range(HEADS):
        values_ref[head, 0:HD, :] = values[head * HD : (head + 1) * HD, :]
        values_ref[head, HD:SUMS, :] = jnp.ones((SUMS - HD, KEYS), bf16)


def each_head(work, heads_step):
    def step(index, carry):
        for one in range(heads_step):
            work(heads_step * index + one)
        return carry

    lax.fori_loop(0, HEADS // heads_step, step, 0)


def attend_kernel(first, refs):
    packed_ref, wv_ref, folded_ref = refs[:3]
    mix_out, keys_ref, values_ref = refs[-3:]
    unpack_keys(packed_ref, keys_ref)
    turn_values(wv_ref, keys_ref, values_ref)

    def work(head):
        weights = jnp.exp2(mm(keys_ref[...], folded_ref[head])).astype(bf16)
        mixed = mm(values_ref[head], weights)
        if not first:
            mixed = mixed + refs[3][head]
        mix_out[head] = mixed

    each_head(work, HEADS_STEP)


def attend_last_kernel(
    packed_ref,
    wv_ref,
    folded_ref,
    mix_ref,
    first_ref,
    second_ref,
    third_ref,
    stay_ref,
    leave_ref,
    keys_ref,
    values_ref,
    total_ref,
    peak_ref,
    blocks_ref,
    scores_ref,
):
    attend_kernel(False, (packed_ref, wv_ref, folded_ref, mix_ref, total_ref, keys_ref, values_ref))
    for head in range(HEADS):
        peak_ref[head] = -folded_ref[head, E:, :].astype(f32)[:8]
    over = jnp.where(jnp.abs(total_ref[...]) < safe_size, 0.0, 1.0)

    @pl.when(jnp.max(over) > 0.0)
    def _():
        for index, one_ref in enumerate((packed_ref, first_ref, second_ref, third_ref)):
            blocks_ref[index] = one_ref[...]
        peak_ref[...] = jnp.full(peak_ref.shape, far_below, f32)
        total_ref[...] = jnp.zeros(total_ref.shape, f32)

        def one_block(index, carry):
            unpack_keys(blocks_ref.at[index], keys_ref)
            turn_values(wv_ref, keys_ref, values_ref)

            def work(head):
                scores_ref[...] = mm(keys_ref[:, :E], folded_ref[head, :E, :])
                old = peak_ref[head][0:1, :]
                peak = jnp.maximum(jnp.max(scores_ref[...], axis=0, keepdims=True), old)
                weights = jnp.exp2(scores_ref[...] - peak).astype(bf16)
                mixed = mm(values_ref[head], weights)
                total_ref[head] = total_ref[head] * jnp.exp2(old - peak) + mixed
                peak_ref[head] = jnp.broadcast_to(peak, (8, ALL_Q))

            each_head(work, 1)
            return carry

        lax.fori_loop(0, SIDE, one_block, 0)

    for head in range(HEADS):
        total = total_ref[head]
        joined = jnp.concatenate(
            [total[: HD + 1], peak_ref[head][0:1, :], total[HD + 2 : STATE]], axis=0
        )
        stay_ref[head] = joined[:, :OWN_Q]
        leave_ref[head] = joined[:, OWN_Q:]


mix_shape = jax.ShapeDtypeStruct((HEADS, SUMS, ALL_Q), f32)
attend_scratch = [pltpu.VMEM((KEYS, FOLD), bf16), pltpu.VMEM((HEADS, SUMS, KEYS), bf16)]
attend_flops = 4 * HEADS * KEYS * ALL_Q * E


def attend(args):
    first = len(args) == 3
    return call(
        lambda *refs: attend_kernel(first, refs),
        [mix_shape],
        args,
        "attend_first" if first else "attend_next",
        attend_flops,
        scratch=attend_scratch,
        limit=28,
    )[0]


def attend_last(args):
    return call(
        attend_last_kernel,
        [jax.ShapeDtypeStruct((HEADS, STATE, OWN_Q), f32)] * 2,
        args,
        "attend_last",
        attend_flops,
        scratch=attend_scratch
        + [
            pltpu.VMEM((HEADS, SUMS, ALL_Q), f32),
            pltpu.VMEM((HEADS, 8, ALL_Q), f32),
            pltpu.VMEM((SIDE, SOURCES * TRAIN_PACK, LANES), bf16),
            pltpu.VMEM((KEYS, ALL_Q), f32),
        ],
        limit=28,
    )


def merge_kernel(stay_ref, came_ref, send_ref):
    parts = []
    for head in range(HEADS):
        stay = stay_ref[head]
        came = came_ref[head]
        peak = jnp.maximum(stay[HD + 1 : HD + 2], came[HD + 1 : HD + 2])
        fade_stay = jnp.exp2(stay[HD + 1 : HD + 2] - peak)
        fade_came = jnp.exp2(came[HD + 1 : HD + 2] - peak)
        total = stay[HD : HD + 1] * fade_stay + came[HD : HD + 1] * fade_came
        mixed = stay[:HD] * fade_stay + came[:HD] * fade_came
        parts.append(mixed / total)
    turned = jnp.concatenate(parts, axis=0).T
    for peer in range(GROUPS):
        send_ref[peer] = pack(turned[peer * ROWS : (peer + 1) * ROWS])


def after_kernel(came_ref, after_ref, wo_ref, up_ref, down_ref, train_ref, test_ref):
    mixes = [unpack(came_ref[index]) for index in range(GROUPS)]
    row_mix = jnp.concatenate(mixes, axis=0).astype(bf16)
    after_row = after_ref[...].reshape(GROUPS * ROWS, E) + mm(row_mix, wo_ref[...])
    third = layer_norm(after_row).astype(bf16)
    raised = mm(third, up_ref[...])
    hidden = (0.5 * raised * (1.0 + lax.erf(raised * (0.5**0.5)))).astype(bf16)
    result = (after_row + mm(hidden, down_ref[...])).astype(bf16)
    for index in range(GROUPS):
        low = index * ROWS
        left = index * E
        train_ref[:, left : left + E] = result[low : low + TRAIN_ROWS]
        test_ref[:, left : left + E] = result[low + TRAIN_ROWS : low + ROWS]


def shift(size, by):
    return [(index, (index + by) % size) for index in range(size)]


def body(train_cells, test_cells, feat_weights, row_weights, mlp_up, mlp_down):
    swap = [(0, 1), (1, 0)]
    joined = jnp.concatenate([train_cells, test_cells], axis=0)
    other = lax.ppermute(joined, "feat", swap)
    wide = (GROUPS * ROWS, E)
    near = call(
        near_kernel,
        [jax.ShapeDtypeStruct((GROUPS, ROWS, E), f32)] + [jax.ShapeDtypeStruct(wide, bf16)] * 3,
        (train_cells, test_cells, feat_weights),
        "near",
        10**9,
    )
    after_feat, pieces = call(
        before_kernel,
        [
            jax.ShapeDtypeStruct((GROUPS, ROWS, E), f32),
            jax.ShapeDtypeStruct((GROUPS, PACK, LANES), bf16),
        ],
        (other, feat_weights, *near),
        "before",
        10**9,
    )
    classes = ("y_lo", "z_lo")
    received = lax.all_to_all(pieces, classes, split_axis=0, concat_axis=0, tiled=True)
    keys = received[:, :TRAIN_PACK].reshape(GROUPS * TRAIN_PACK, LANES)
    column = [keys] + [lax.ppermute(keys, "z_hi", shift(SIDE, by)) for by in (1, 3, 2)]
    received_other = lax.ppermute(received, "core", swap)
    folded = call(
        fold_kernel,
        [jax.ShapeDtypeStruct((HEADS, FOLD, ALL_Q), bf16)],
        (received, received_other, row_weights),
        "fold",
        10**9,
    )[0]
    column, folded = lax.optimization_barrier((column, folded))
    keys = jnp.concatenate(column, axis=0)
    value_turned = row_weights[2].T
    distant = [lax.ppermute(keys, "x", shift(4, by)) for by in (1, 3)]
    mix = attend((keys, value_turned, folded))
    keys, mix = lax.optimization_barrier((keys, mix))
    distant.append(lax.ppermute(keys, "x", shift(4, 2)))
    for one in distant[:-1]:
        mix = attend((one, value_turned, folded, mix))
    stay, leave = attend_last(
        (distant[-1], value_turned, folded, mix, keys, distant[0], distant[1])
    )
    came = lax.ppermute(leave, "core", swap)
    mixed = call(
        merge_kernel,
        [jax.ShapeDtypeStruct((GROUPS, PACK, LANES), bf16)],
        (stay, came),
        "merge",
        10**7,
    )[0]
    returned = lax.all_to_all(mixed, classes, split_axis=0, concat_axis=0, tiled=True)
    train_out, test_out = call(
        after_kernel,
        [
            jax.ShapeDtypeStruct((TRAIN_ROWS, GROUPS * E), bf16),
            jax.ShapeDtypeStruct((TEST_ROWS, GROUPS * E), bf16),
        ],
        (returned, after_feat, row_weights[3], mlp_up, mlp_down),
        "after",
        10**9,
    )
    return (train_out, test_out)


def solution(mesh):
    split = Mesh(
        mesh.devices.reshape(2, 4, 4, 2, 2, 2), ("y_lo", "x", "z_hi", "z_lo", "core", "feat")
    )
    rows = ("y_lo", "x", "z_hi", "z_lo", "core")
    return jax.shard_map(
        body,
        mesh=split,
        in_specs=(P(rows, "feat"), P(rows, "feat"), P(), P(), P(), P()),
        out_specs=(P(rows, "feat"), P(rows, "feat")),
        check_vma=False,
    )
```

```python
import math

import jax
import jax.numpy as jnp
from jax import lax
from jax.experimental import pallas as pl
from jax.experimental.pallas import tpu as pltpu
from jax.sharding import Mesh
from jax.sharding import PartitionSpec as P

E = 192
HEADS = 6
HD = 32
HID = 768
GROUPS = 4
FEATS = 8
TRAIN_ROWS = 64
TEST_ROWS = 32
ROWS = TRAIN_ROWS + TEST_ROWS
SIDE = 4
LANES = 128
REST = E - LANES
TRAIN_PACK = TRAIN_ROWS + TRAIN_ROWS // 2
PACK = ROWS + ROWS // 2
OWN_Q = GROUPS * ROWS
ALL_Q = 2 * OWN_Q
SOURCES = GROUPS * SIDE
KEYS = SOURCES * TRAIN_ROWS
SUMS = HD + 16
FOLD = E + 16
PROBES = 64
HEADS_STEP = 3
STATE = HD + 8

eps_norm = 1e-05
far_below = -3e38
safe_size = 2.0**60
log2_scale = HD ** (-0.5) * math.log2(math.e)


bf16 = jnp.bfloat16
f32 = jnp.float32


def mm(left, right):
    return jnp.dot(left, right, preferred_element_type=f32)


def mm_nt(left, right):
    return lax.dot_general(left, right, (((1,), (1,)), ((), ())), preferred_element_type=f32)


def layer_norm(values_in):
    centred = values_in - jnp.mean(values_in, axis=-1, keepdims=True)
    spread = jnp.mean(centred * centred, axis=-1, keepdims=True)
    return centred * lax.rsqrt(spread + eps_norm)


def call(kernel, outs, args, name, flops, scratch=(), limit=12):
    in_vmem = pl.BlockSpec(memory_space=pltpu.VMEM)
    return pl.pallas_call(
        kernel,
        out_shape=outs,
        in_specs=[in_vmem] * len(args),
        out_specs=[in_vmem] * len(outs),
        scratch_shapes=list(scratch),
        compiler_params=pltpu.CompilerParams(vmem_limit_bytes=limit * 2**20),
        cost_estimate=pl.CostEstimate(flops=flops, transcendentals=0, bytes_accessed=2**20),
        name=name,
    )(*args)


def pack_rows(rows):
    half = rows.shape[0] // 2
    rest = rows[:, LANES:]
    return [rows[:, :LANES], jnp.concatenate([rest[:half], rest[half:]], axis=1)]


def pack(rows):
    parts = pack_rows(rows[:TRAIN_ROWS]) + pack_rows(rows[TRAIN_ROWS:])
    return jnp.concatenate(parts, axis=0).astype(bf16)


def unpack_rows(packed):
    height = packed.shape[0] * 2 // 3
    rest = packed[height:]
    rest = jnp.concatenate([rest[:, :REST], rest[:, REST:]], axis=0)
    return jnp.concatenate([packed[:height], rest], axis=1)


def unpack(packed):
    packed = packed.astype(f32)
    parts = [unpack_rows(packed[:TRAIN_PACK]), unpack_rows(packed[TRAIN_PACK:])]
    return jnp.concatenate(parts, axis=0)


def near_kernel(train_ref, test_ref, weights_ref, cells_ref, query_ref, key_ref, value_ref):
    parts = []
    for index in range(GROUPS):
        span = slice(index * E, (index + 1) * E)
        cell = [one_ref[:, span].astype(f32) for one_ref in (train_ref, test_ref)]
        cell = jnp.concatenate(cell, axis=0)
        cells_ref[index] = cell
        parts.append(layer_norm(cell).astype(bf16))
    normed = jnp.concatenate(parts, axis=0)
    query_ref[...] = (mm(normed, weights_ref[0]) * log2_scale).astype(bf16)
    key_ref[...] = mm(normed, weights_ref[1]).astype(bf16)
    value_ref[...] = mm(normed, weights_ref[2]).astype(bf16)


def before_kernel(
    other_ref, weights_ref, cells_ref, query_ref, key_ref, value_ref, after_ref, send_ref
):
    parts = []
    for index in range(GROUPS):
        cell = other_ref[:, index * E : (index + 1) * E].astype(f32)
        parts.append(layer_norm(cell).astype(bf16))
    normed = jnp.concatenate(parts, axis=0)
    far_keys = mm(normed, weights_ref[1]).astype(bf16)
    far_values = mm(normed, weights_ref[2]).astype(bf16)
    queries = query_ref[...]
    keys = jnp.concatenate([key_ref[...], far_keys], axis=0)
    values = jnp.concatenate([value_ref[...], far_values], axis=0).astype(f32)
    head_of = lax.broadcasted_iota(jnp.int32, (E, 128), 0) >> 5
    gather = jnp.where(head_of == lax.broadcasted_iota(jnp.int32, (E, 128), 1), 1.0, 0.0).astype(bf16)
    head_to = lax.broadcasted_iota(jnp.int32, (128, E), 1) >> 5
    spread = jnp.where(head_to == lax.broadcasted_iota(jnp.int32, (128, E), 0), 1.0, 0.0).astype(bf16)
    mixtures = []
    for index in range(GROUPS):
        asked = queries[index * ROWS : (index + 1) * ROWS]
        products = jnp.concatenate(
            [asked * keys[j * ROWS : (j + 1) * ROWS] for j in range(FEATS)], axis=0
        )
        scores = mm(products, gather)
        pieces = [scores[j * ROWS : (j + 1) * ROWS] for j in range(FEATS)]
        peak = pieces[0]
        for one in pieces[1:]:
            peak = jnp.maximum(peak, one)
        weights = [jnp.exp2(one - peak) for one in pieces]
        total = weights[0]
        for one in weights[1:]:
            total = total + one
        high = total.astype(bf16)
        low = (total - high.astype(f32)).astype(bf16)
        wide = mm(jnp.concatenate([one.astype(bf16) for one in weights] + [high, low], axis=0), spread)
        mixed = wide[:ROWS] * values[:ROWS]
        for j in range(1, FEATS):
            mixed = mixed + wide[j * ROWS : (j + 1) * ROWS] * values[j * ROWS : (j + 1) * ROWS]
        whole = wide[FEATS * ROWS : (FEATS + 1) * ROWS] + wide[(FEATS + 1) * ROWS :]
        mixtures.append((mixed / whole).astype(bf16))
    moved = mm(jnp.concatenate(mixtures, axis=0), weights_ref[3]).astype(bf16).astype(f32)
    for index in range(GROUPS):
        after = cells_ref[index] + moved[index * ROWS : (index + 1) * ROWS]
        after_ref[index] = after
        send_ref[index] = pack(layer_norm(after))


def fold_kernel(own_ref, other_ref, weights_ref, folded_ref, turned_ref):
    turned_ref[...] = weights_ref[2].astype(f32).T.astype(bf16)
    parts = [unpack(one_ref[index]) for one_ref in (own_ref, other_ref) for index in range(GROUPS)]
    asked = jnp.concatenate(parts, axis=0).astype(bf16)
    probes = jnp.concatenate([parts[0][:PROBES], parts[GROUPS][:PROBES]], axis=0).astype(bf16)
    queries = (mm(asked, weights_ref[0]) * log2_scale).astype(bf16)
    weight = weights_ref[1]
    row = lax.broadcasted_iota(jnp.int32, (FOLD - E, ALL_Q), 0)
    for head in range(HEADS):
        part = slice(head * HD, (head + 1) * HD)
        folded = mm_nt(weight[:, part], queries[:, part]).astype(bf16)
        peak = jnp.max(mm(probes, folded), axis=0, keepdims=True)
        folded_ref[head, :E, :] = folded
        folded_ref[head, E:, :] = jnp.where(row == 0, -peak, 0.0).astype(bf16)


def stack_kernel(*refs):
    height = GROUPS * TRAIN_PACK
    for index in range(SIDE):
        refs[-1][index * height : (index + 1) * height, :] = refs[index][...]


def unpack_keys(packed_ref, keys_ref):
    half = TRAIN_ROWS // 2
    for source in range(SOURCES):
        low = source * TRAIN_ROWS
        top = source * TRAIN_PACK
        rest = packed_ref[top + TRAIN_ROWS : top + TRAIN_PACK, :]
        keys_ref[low : low + TRAIN_ROWS, :LANES] = packed_ref[top : top + TRAIN_ROWS, :]
        keys_ref[low : low + half, LANES:E] = rest[:, :REST]
        keys_ref[low + half : low + TRAIN_ROWS, LANES:E] = rest[:, REST:]
    keys_ref[:, E:] = jnp.ones((KEYS, FOLD - E), bf16)


def turn_values(wv_ref, keys_ref, values_ref):
    values = mm_nt(wv_ref[...], keys_ref[:, :E]).astype(bf16)
    for head in range(HEADS):
        values_ref[head, 0:HD, :] = values[head * HD : (head + 1) * HD, :]
        values_ref[head, HD:SUMS, :] = jnp.ones((SUMS - HD, KEYS), bf16)


def each_head(work, heads_step):
    def step(index, carry):
        for one in range(heads_step):
            work(heads_step * index + one)
        return carry

    lax.fori_loop(0, HEADS // heads_step, step, 0)


def attend_kernel(first, refs):
    packed_ref, wv_ref, folded_ref = refs[:3]
    mix_out, keys_ref, values_ref = refs[-3:]
    unpack_keys(packed_ref, keys_ref)
    turn_values(wv_ref, keys_ref, values_ref)

    def work(head):
        weights = jnp.exp2(mm(keys_ref[...], folded_ref[head])).astype(bf16)
        mixed = mm(values_ref[head], weights)
        if not first:
            mixed = mixed + refs[3][head]
        mix_out[head] = mixed

    each_head(work, HEADS_STEP)


def attend_last_kernel(
    packed_ref,
    wv_ref,
    folded_ref,
    mix_ref,
    first_ref,
    second_ref,
    third_ref,
    stay_ref,
    leave_ref,
    keys_ref,
    values_ref,
    total_ref,
    peak_ref,
    blocks_ref,
    scores_ref,
):
    attend_kernel(False, (packed_ref, wv_ref, folded_ref, mix_ref, total_ref, keys_ref, values_ref))
    for head in range(HEADS):
        peak_ref[head] = -folded_ref[head, E:, :].astype(f32)[:8]
    over = jnp.where(jnp.abs(total_ref[...]) < safe_size, 0.0, 1.0)

    @pl.when(jnp.max(over) > 0.0)
    def _():
        for index, one_ref in enumerate((packed_ref, first_ref, second_ref, third_ref)):
            blocks_ref[index] = one_ref[...]
        peak_ref[...] = jnp.full(peak_ref.shape, far_below, f32)
        total_ref[...] = jnp.zeros(total_ref.shape, f32)

        def one_block(index, carry):
            unpack_keys(blocks_ref.at[index], keys_ref)
            turn_values(wv_ref, keys_ref, values_ref)

            def work(head):
                scores_ref[...] = mm(keys_ref[:, :E], folded_ref[head, :E, :])
                old = peak_ref[head][0:1, :]
                peak = jnp.maximum(jnp.max(scores_ref[...], axis=0, keepdims=True), old)
                weights = jnp.exp2(scores_ref[...] - peak).astype(bf16)
                mixed = mm(values_ref[head], weights)
                total_ref[head] = total_ref[head] * jnp.exp2(old - peak) + mixed
                peak_ref[head] = jnp.broadcast_to(peak, (8, ALL_Q))

            each_head(work, 1)
            return carry

        lax.fori_loop(0, SIDE, one_block, 0)

    for head in range(HEADS):
        total = total_ref[head]
        joined = jnp.concatenate(
            [total[: HD + 1], peak_ref[head][0:1, :], total[HD + 2 : STATE]], axis=0
        )
        stay_ref[head] = joined[:, :OWN_Q]
        leave_ref[head] = joined[:, OWN_Q:]


mix_shape = jax.ShapeDtypeStruct((HEADS, SUMS, ALL_Q), f32)
attend_scratch = [pltpu.VMEM((KEYS, FOLD), bf16), pltpu.VMEM((HEADS, SUMS, KEYS), bf16)]
attend_flops = 4 * HEADS * KEYS * ALL_Q * E


def attend(args):
    first = len(args) == 3
    return call(
        lambda *refs: attend_kernel(first, refs),
        [mix_shape],
        args,
        "attend_first" if first else "attend_next",
        attend_flops,
        scratch=attend_scratch,
        limit=20,
    )[0]


def attend_last(args):
    return call(
        attend_last_kernel,
        [jax.ShapeDtypeStruct((HEADS, STATE, OWN_Q), f32)] * 2,
        args,
        "attend_last",
        attend_flops,
        scratch=attend_scratch
        + [
            pltpu.VMEM((HEADS, SUMS, ALL_Q), f32),
            pltpu.VMEM((HEADS, 8, ALL_Q), f32),
            pltpu.VMEM((SIDE, SOURCES * TRAIN_PACK, LANES), bf16),
            pltpu.VMEM((KEYS, ALL_Q), f32),
        ],
        limit=20,
    )


def merge_kernel(stay_ref, came_ref, send_ref):
    parts = []
    for head in range(HEADS):
        stay = stay_ref[head]
        came = came_ref[head]
        peak = jnp.maximum(stay[HD + 1 : HD + 2], came[HD + 1 : HD + 2])
        fade_stay = jnp.exp2(stay[HD + 1 : HD + 2] - peak)
        fade_came = jnp.exp2(came[HD + 1 : HD + 2] - peak)
        total = stay[HD : HD + 1] * fade_stay + came[HD : HD + 1] * fade_came
        mixed = stay[:HD] * fade_stay + came[:HD] * fade_came
        parts.append(mixed / total)
    turned = jnp.concatenate(parts, axis=0).T
    for peer in range(GROUPS):
        send_ref[peer] = pack(turned[peer * ROWS : (peer + 1) * ROWS])


def after_kernel(came_ref, after_ref, wo_ref, up_ref, down_ref, train_ref, test_ref):
    mixes = [unpack(came_ref[index]) for index in range(GROUPS)]
    row_mix = jnp.concatenate(mixes, axis=0).astype(bf16)
    after_row = after_ref[...].reshape(GROUPS * ROWS, E) + mm(row_mix, wo_ref[...])
    third = layer_norm(after_row).astype(bf16)
    raised = mm(third, up_ref[...])
    hidden = (0.5 * raised * (1.0 + lax.erf(raised * (0.5**0.5)))).astype(bf16)
    result = (after_row + mm(hidden, down_ref[...])).astype(bf16)
    for index in range(GROUPS):
        low = index * ROWS
        left = index * E
        train_ref[:, left : left + E] = result[low : low + TRAIN_ROWS]
        test_ref[:, left : left + E] = result[low + TRAIN_ROWS : low + ROWS]


def shift(size, by):
    return [(index, (index + by) % size) for index in range(size)]


def body(train_cells, test_cells, feat_weights, row_weights, mlp_up, mlp_down):
    swap = [(0, 1), (1, 0)]
    joined = jnp.concatenate([train_cells, test_cells], axis=0)
    other = lax.ppermute(joined, "feat", swap)
    wide = (GROUPS * ROWS, E)
    near = call(
        near_kernel,
        [jax.ShapeDtypeStruct((GROUPS, ROWS, E), f32)] + [jax.ShapeDtypeStruct(wide, bf16)] * 3,
        (train_cells, test_cells, feat_weights),
        "near",
        10**9,
    )
    after_feat, pieces = call(
        before_kernel,
        [
            jax.ShapeDtypeStruct((GROUPS, ROWS, E), f32),
            jax.ShapeDtypeStruct((GROUPS, PACK, LANES), bf16),
        ],
        (other, feat_weights, *near),
        "before",
        10**9,
    )
    classes = ("y_lo", "z_lo")
    received = lax.all_to_all(pieces, classes, split_axis=0, concat_axis=0, tiled=True)
    keys = received[:, :TRAIN_PACK].reshape(GROUPS * TRAIN_PACK, LANES)
    column = [keys] + [lax.ppermute(keys, "z_hi", shift(SIDE, by)) for by in (1, 3, 2)]
    received_other = lax.ppermute(received, "core", swap)
    folded, value_turned = call(
        fold_kernel,
        [
            jax.ShapeDtypeStruct((HEADS, FOLD, ALL_Q), bf16),
            jax.ShapeDtypeStruct((E, E), bf16),
        ],
        (received, received_other, row_weights),
        "fold",
        10**9,
    )
    column, folded = lax.optimization_barrier((column, folded))
    keys = call(
        stack_kernel,
        [jax.ShapeDtypeStruct((SIDE * GROUPS * TRAIN_PACK, LANES), bf16)],
        column,
        "stack",
        10**6,
        limit=4,
    )[0]
    distant = [lax.ppermute(keys, "x", shift(4, by)) for by in (1, 3, 2)]
    mix = attend((keys, value_turned, folded))
    for one in distant[:-1]:
        mix = attend((one, value_turned, folded, mix))
    stay, leave = attend_last(
        (distant[-1], value_turned, folded, mix, keys, distant[0], distant[1])
    )
    came = lax.ppermute(leave, "core", swap)
    mixed = call(
        merge_kernel,
        [jax.ShapeDtypeStruct((GROUPS, PACK, LANES), bf16)],
        (stay, came),
        "merge",
        10**7,
    )[0]
    returned = lax.all_to_all(mixed, classes, split_axis=0, concat_axis=0, tiled=True)
    train_out, test_out = call(
        after_kernel,
        [
            jax.ShapeDtypeStruct((TRAIN_ROWS, GROUPS * E), bf16),
            jax.ShapeDtypeStruct((TEST_ROWS, GROUPS * E), bf16),
        ],
        (returned, after_feat, row_weights[3], mlp_up, mlp_down),
        "after",
        10**9,
    )
    return (train_out, test_out)


def solution(mesh):
    split = Mesh(
        mesh.devices.reshape(2, 4, 4, 2, 2, 2), ("y_lo", "x", "z_hi", "z_lo", "core", "feat")
    )
    rows = ("y_lo", "x", "z_hi", "z_lo", "core")
    return jax.shard_map(
        body,
        mesh=split,
        in_specs=(P(rows, "feat"), P(rows, "feat"), P(), P(), P(), P()),
        out_specs=(P(rows, "feat"), P(rows, "feat")),
        check_vma=False,
    )
```

```python
import math

import jax
import jax.numpy as jnp
from jax import lax
from jax.experimental import pallas as pl
from jax.experimental.pallas import tpu as pltpu
from jax.sharding import Mesh
from jax.sharding import PartitionSpec as P

E = 192
HEADS = 6
HD = 32
GROUPS = 4
FEATS = 8
TRAIN_ROWS = 64
TEST_ROWS = 32
ROWS = TRAIN_ROWS + TEST_ROWS
SIDE = 4
LANES = 128
REST = E - LANES
TRAIN_PACK = TRAIN_ROWS + TRAIN_ROWS // 2
PACK = ROWS + ROWS // 2
OWN_Q = GROUPS * ROWS
ALL_Q = 2 * OWN_Q
SOURCES = GROUPS * SIDE
KEYS = SOURCES * TRAIN_ROWS
SUMS = HD + 16
FOLD = E + 16
PROBES = 64
BLOCK = SOURCES * TRAIN_PACK
STATE = HD + 8

eps_norm = 1e-05
far_below = -3e38
safe_size = 2.0**60
log2_scale = HD ** (-0.5) * math.log2(math.e)


bf16 = jnp.bfloat16
f32 = jnp.float32


def mm(left, right):
    return jnp.dot(left, right, preferred_element_type=f32)


def mm_nt(left, right):
    return lax.dot_general(left, right, (((1,), (1,)), ((), ())), preferred_element_type=f32)


def layer_norm(values_in):
    centred = values_in - jnp.mean(values_in, axis=-1, keepdims=True)
    spread = jnp.mean(centred * centred, axis=-1, keepdims=True)
    return centred * lax.rsqrt(spread + eps_norm)


def call(kernel, outs, args, flops, scratch=(), limit=12):
    in_vmem = pl.BlockSpec(memory_space=pltpu.VMEM)
    return pl.pallas_call(
        kernel,
        out_shape=outs,
        in_specs=[in_vmem] * len(args),
        out_specs=[in_vmem] * len(outs),
        scratch_shapes=list(scratch),
        compiler_params=pltpu.CompilerParams(vmem_limit_bytes=limit * 2**20),
        cost_estimate=pl.CostEstimate(flops=flops, transcendentals=0, bytes_accessed=2**20),
    )(*args)


def pack_rows(rows):
    half = rows.shape[0] // 2
    rest = rows[:, LANES:]
    return [rows[:, :LANES], jnp.concatenate([rest[:half], rest[half:]], axis=1)]


def pack(rows):
    parts = pack_rows(rows[:TRAIN_ROWS]) + pack_rows(rows[TRAIN_ROWS:])
    return jnp.concatenate(parts, axis=0).astype(bf16)


def unpack_rows(packed):
    height = packed.shape[0] * 2 // 3
    rest = packed[height:]
    rest = jnp.concatenate([rest[:, :REST], rest[:, REST:]], axis=0)
    return jnp.concatenate([packed[:height], rest], axis=1)


def unpack(packed):
    packed = packed.astype(f32)
    parts = [unpack_rows(packed[:TRAIN_PACK]), unpack_rows(packed[TRAIN_PACK:])]
    return jnp.concatenate(parts, axis=0)


def near_kernel(train_ref, test_ref, weights_ref, cells_ref, query_ref, key_ref, value_ref):
    parts = []
    for index in range(GROUPS):
        span = slice(index * E, (index + 1) * E)
        cell = [one_ref[:, span].astype(f32) for one_ref in (train_ref, test_ref)]
        cell = jnp.concatenate(cell, axis=0)
        cells_ref[index] = cell
        parts.append(layer_norm(cell).astype(bf16))
    normed = jnp.concatenate(parts, axis=0)
    query_ref[...] = (mm(normed, weights_ref[0]) * log2_scale).astype(bf16)
    key_ref[...] = mm(normed, weights_ref[1]).astype(bf16)
    value_ref[...] = mm(normed, weights_ref[2]).astype(bf16)


def before_kernel(
    other_ref, weights_ref, cells_ref, query_ref, key_ref, value_ref, after_ref, send_ref
):
    parts = []
    for index in range(GROUPS):
        cell = other_ref[:, index * E : (index + 1) * E].astype(f32)
        parts.append(layer_norm(cell).astype(bf16))
    normed = jnp.concatenate(parts, axis=0)
    far_keys = mm(normed, weights_ref[1]).astype(bf16)
    far_values = mm(normed, weights_ref[2]).astype(bf16)
    queries = query_ref[...]
    keys = jnp.concatenate([key_ref[...], far_keys], axis=0)
    values = jnp.concatenate([value_ref[...], far_values], axis=0).astype(f32)
    head_of = lax.broadcasted_iota(jnp.int32, (E, 128), 0) >> 5
    gather = jnp.where(head_of == lax.broadcasted_iota(jnp.int32, (E, 128), 1), 1.0, 0.0).astype(bf16)
    head_to = lax.broadcasted_iota(jnp.int32, (128, E), 1) >> 5
    spread = jnp.where(head_to == lax.broadcasted_iota(jnp.int32, (128, E), 0), 1.0, 0.0).astype(bf16)
    mixtures = []
    for index in range(GROUPS):
        asked = queries[index * ROWS : (index + 1) * ROWS]
        products = jnp.concatenate(
            [asked * keys[j * ROWS : (j + 1) * ROWS] for j in range(FEATS)], axis=0
        )
        scores = mm(products, gather)
        pieces = [scores[j * ROWS : (j + 1) * ROWS] for j in range(FEATS)]
        peak = pieces[0]
        for one in pieces[1:]:
            peak = jnp.maximum(peak, one)
        weights = [jnp.exp2(one - peak) for one in pieces]
        total = weights[0]
        for one in weights[1:]:
            total = total + one
        high = total.astype(bf16)
        low = (total - high.astype(f32)).astype(bf16)
        wide = mm(jnp.concatenate([one.astype(bf16) for one in weights] + [high, low], axis=0), spread)
        mixed = wide[:ROWS] * values[:ROWS]
        for j in range(1, FEATS):
            mixed = mixed + wide[j * ROWS : (j + 1) * ROWS] * values[j * ROWS : (j + 1) * ROWS]
        whole = wide[FEATS * ROWS : (FEATS + 1) * ROWS] + wide[(FEATS + 1) * ROWS :]
        mixtures.append((mixed / whole).astype(bf16))
    moved = mm(jnp.concatenate(mixtures, axis=0), weights_ref[3]).astype(bf16).astype(f32)
    for index in range(GROUPS):
        after = cells_ref[index] + moved[index * ROWS : (index + 1) * ROWS]
        after_ref[index] = after
        send_ref[index] = pack(layer_norm(after))


def fold_kernel(own_ref, other_ref, weights_ref, folded_ref, turned_ref):
    turned_ref[...] = weights_ref[2].astype(f32).T.astype(bf16)
    parts = [unpack(one_ref[index]) for one_ref in (own_ref, other_ref) for index in range(GROUPS)]
    asked = jnp.concatenate(parts, axis=0).astype(bf16)
    probes = jnp.concatenate([parts[0][:PROBES], parts[GROUPS][:PROBES]], axis=0).astype(bf16)
    queries = (mm(asked, weights_ref[0]) * log2_scale).astype(bf16)
    weight = weights_ref[1]
    row = lax.broadcasted_iota(jnp.int32, (FOLD - E, ALL_Q), 0)
    for head in range(HEADS):
        part = slice(head * HD, (head + 1) * HD)
        folded = mm_nt(weight[:, part], queries[:, part]).astype(bf16)
        peak = jnp.max(mm(probes, folded), axis=0, keepdims=True)
        folded_ref[head, :E, :] = folded
        folded_ref[head, E:, :] = jnp.where(row == 0, -peak, 0.0).astype(bf16)


def stack_kernel(*refs):
    height = GROUPS * TRAIN_PACK
    for index in range(SIDE):
        refs[-1][index * height : (index + 1) * height, :] = refs[index][...]


def unpack_keys(packed_refs, keys_ref):
    half = TRAIN_ROWS // 2
    each = SOURCES // len(packed_refs)
    for source in range(SOURCES):
        packed_ref = packed_refs[source // each]
        low = source * TRAIN_ROWS
        top = source % each * TRAIN_PACK
        rest = packed_ref[top + TRAIN_ROWS : top + TRAIN_PACK, :]
        keys_ref[low : low + TRAIN_ROWS, :LANES] = packed_ref[top : top + TRAIN_ROWS, :]
        keys_ref[low : low + half, LANES:E] = rest[:, :REST]
        keys_ref[low + half : low + TRAIN_ROWS, LANES:E] = rest[:, REST:]
    keys_ref[:, E:] = jnp.ones((KEYS, FOLD - E), bf16)


def turn_values(wv_ref, keys_ref, values_ref):
    values = mm_nt(wv_ref[...], keys_ref[:, :E]).astype(bf16)
    for head in range(HEADS):
        values_ref[head, 0:HD, :] = values[head * HD : (head + 1) * HD, :]
        values_ref[head, HD:SUMS, :] = jnp.ones((SUMS - HD, KEYS), bf16)


def attend_kernel(first, packed_refs, refs):
    wv_ref, folded_ref = refs[:2]
    mix_out, keys_ref, values_ref = refs[-3:]
    unpack_keys(packed_refs, keys_ref)
    turn_values(wv_ref, keys_ref, values_ref)

    def work(head):
        weights = jnp.exp2(mm(keys_ref[...], folded_ref[head])).astype(bf16)
        mixed = mm(values_ref[head], weights)
        if not first:
            mixed = mixed + refs[2][head]
        mix_out[head] = mixed

    for head in range(HEADS):
        work(head)


def attend_last_kernel(
    left_ref,
    right_ref,
    wv_ref,
    folded_ref,
    mix_ref,
    first_ref,
    second_ref,
    third_ref,
    stay_ref,
    leave_ref,
    keys_ref,
    values_ref,
    total_ref,
    peak_ref,
    blocks_ref,
    scores_ref,
):
    attend_kernel(
        False,
        (left_ref, right_ref),
        (wv_ref, folded_ref, mix_ref, total_ref, keys_ref, values_ref),
    )
    for head in range(HEADS):
        peak_ref[head] = -folded_ref[head, E:, :].astype(f32)[:8]
    over = jnp.where(jnp.abs(total_ref[...]) < safe_size, 0.0, 1.0)

    @pl.when(jnp.max(over) > 0.0)
    def _():
        for index, one_ref in enumerate((first_ref, second_ref, third_ref)):
            blocks_ref[index] = one_ref[...]
        blocks_ref[SIDE - 1, : BLOCK // 2] = left_ref[...]
        blocks_ref[SIDE - 1, BLOCK // 2 :] = right_ref[...]
        peak_ref[...] = jnp.full(peak_ref.shape, far_below, f32)
        total_ref[...] = jnp.zeros(total_ref.shape, f32)

        def one_block(index, carry):
            unpack_keys((blocks_ref.at[index],), keys_ref)
            turn_values(wv_ref, keys_ref, values_ref)

            def work(head, kept):
                scores_ref[...] = mm(keys_ref[:, :E], folded_ref[head, :E, :])
                old = peak_ref[head][0:1, :]
                peak = jnp.maximum(jnp.max(scores_ref[...], axis=0, keepdims=True), old)
                weights = jnp.exp2(scores_ref[...] - peak).astype(bf16)
                mixed = mm(values_ref[head], weights)
                total_ref[head] = total_ref[head] * jnp.exp2(old - peak) + mixed
                peak_ref[head] = jnp.broadcast_to(peak, (8, ALL_Q))
                return kept

            lax.fori_loop(0, HEADS, work, 0)
            return carry

        lax.fori_loop(0, SIDE, one_block, 0)

    for head in range(HEADS):
        total = total_ref[head]
        joined = jnp.concatenate(
            [total[: HD + 1], peak_ref[head][0:1, :], total[HD + 2 : STATE]], axis=0
        )
        stay_ref[head] = joined[:, :OWN_Q]
        leave_ref[head] = joined[:, OWN_Q:]


mix_shape = jax.ShapeDtypeStruct((HEADS, SUMS, ALL_Q), f32)
attend_scratch = [pltpu.VMEM((KEYS, FOLD), bf16), pltpu.VMEM((HEADS, SUMS, KEYS), bf16)]
attend_flops = 4 * HEADS * KEYS * ALL_Q * E


def attend(args):
    first = len(args) == 3
    return call(
        lambda *refs: attend_kernel(first, refs[:1], refs[1:]),
        [mix_shape],
        args,
        attend_flops,
        scratch=attend_scratch,
        limit=20,
    )[0]


def attend_last(args):
    return call(
        attend_last_kernel,
        [jax.ShapeDtypeStruct((HEADS, STATE, OWN_Q), f32)] * 2,
        args,
        attend_flops,
        scratch=attend_scratch
        + [
            pltpu.VMEM((HEADS, SUMS, ALL_Q), f32),
            pltpu.VMEM((HEADS, 8, ALL_Q), f32),
            pltpu.VMEM((SIDE, BLOCK, LANES), bf16),
            pltpu.VMEM((KEYS, ALL_Q), f32),
        ],
        limit=20,
    )


def merge_kernel(stay_ref, came_ref, send_ref):
    parts = []
    for head in range(HEADS):
        stay = stay_ref[head]
        came = came_ref[head]
        peak = jnp.maximum(stay[HD + 1 : HD + 2], came[HD + 1 : HD + 2])
        fade_stay = jnp.exp2(stay[HD + 1 : HD + 2] - peak)
        fade_came = jnp.exp2(came[HD + 1 : HD + 2] - peak)
        total = stay[HD : HD + 1] * fade_stay + came[HD : HD + 1] * fade_came
        mixed = stay[:HD] * fade_stay + came[:HD] * fade_came
        parts.append(mixed / total)
    turned = jnp.concatenate(parts, axis=0).T
    for peer in range(GROUPS):
        send_ref[peer] = pack(turned[peer * ROWS : (peer + 1) * ROWS])


def after_kernel(came_ref, after_ref, wo_ref, up_ref, down_ref, train_ref, test_ref):
    mixes = [unpack(came_ref[index]) for index in range(GROUPS)]
    row_mix = jnp.concatenate(mixes, axis=0).astype(bf16)
    after_row = after_ref[...].reshape(GROUPS * ROWS, E) + mm(row_mix, wo_ref[...])
    third = layer_norm(after_row).astype(bf16)
    raised = mm(third, up_ref[...])
    hidden = (0.5 * raised * (1.0 + lax.erf(raised * (0.5**0.5)))).astype(bf16)
    result = (after_row + mm(hidden, down_ref[...])).astype(bf16)
    for index in range(GROUPS):
        low = index * ROWS
        left = index * E
        train_ref[:, left : left + E] = result[low : low + TRAIN_ROWS]
        test_ref[:, left : left + E] = result[low + TRAIN_ROWS : low + ROWS]


def shift(size, by):
    return [(index, (index + by) % size) for index in range(size)]


def layer(train_cells, test_cells, feat_weights, row_weights, mlp_up, mlp_down):
    swap = [(0, 1), (1, 0)]
    joined = jnp.concatenate([train_cells, test_cells], axis=0)
    other = lax.ppermute(joined, "feat", swap)
    wide = (GROUPS * ROWS, E)
    near = call(
        near_kernel,
        [jax.ShapeDtypeStruct((GROUPS, ROWS, E), f32)] + [jax.ShapeDtypeStruct(wide, bf16)] * 3,
        (train_cells, test_cells, feat_weights),
        10**9,
    )
    after_feat, pieces = call(
        before_kernel,
        [
            jax.ShapeDtypeStruct((GROUPS, ROWS, E), f32),
            jax.ShapeDtypeStruct((GROUPS, PACK, LANES), bf16),
        ],
        (other, feat_weights, *near),
        10**9,
    )
    classes = ("y_lo", "z_lo")
    received = lax.all_to_all(pieces, classes, split_axis=0, concat_axis=0, tiled=True)
    keys = received[:, :TRAIN_PACK].reshape(GROUPS * TRAIN_PACK, LANES)
    column = [keys]
    for by in (1, 3, 2):
        column.append(lax.ppermute(keys, "z_hi", shift(SIDE, by)))
    received_other = lax.ppermute(received, "core", swap)
    folded, value_turned = call(
        fold_kernel,
        [
            jax.ShapeDtypeStruct((HEADS, FOLD, ALL_Q), bf16),
            jax.ShapeDtypeStruct((E, E), bf16),
        ],
        (received, received_other, row_weights),
        10**9,
    )
    column, folded = lax.optimization_barrier((column, folded))
    keys = call(
        stack_kernel,
        [jax.ShapeDtypeStruct((SIDE * GROUPS * TRAIN_PACK, LANES), bf16)],
        column,
        10**6,
        limit=4,
    )[0]
    above = lax.ppermute(keys, "x", shift(4, 1))
    below = lax.ppermute(keys, "x", shift(4, 3))
    mix = attend((keys, value_turned, folded))
    mix, above, below = lax.optimization_barrier((mix, above, below))
    far_above = lax.ppermute(above[: BLOCK // 2], "x", shift(4, 1))
    far_below_keys = lax.ppermute(below[BLOCK // 2 :], "x", shift(4, 3))
    mix = attend((above, value_turned, folded, mix))
    mix = attend((below, value_turned, folded, mix))
    stay, leave = attend_last(
        (far_above, far_below_keys, value_turned, folded, mix, keys, above, below)
    )
    came = lax.ppermute(leave, "core", swap)
    mixed = call(
        merge_kernel, [jax.ShapeDtypeStruct((GROUPS, PACK, LANES), bf16)], (stay, came), 10**7
    )[0]
    returned = lax.all_to_all(mixed, classes, split_axis=0, concat_axis=0, tiled=True)
    train_out, test_out = call(
        after_kernel,
        [
            jax.ShapeDtypeStruct((TRAIN_ROWS, GROUPS * E), bf16),
            jax.ShapeDtypeStruct((TEST_ROWS, GROUPS * E), bf16),
        ],
        (returned, after_feat, row_weights[3], mlp_up, mlp_down),
        10**9,
    )
    return (train_out, test_out)


def solution(mesh):
    split = Mesh(
        mesh.devices.reshape(2, 4, 4, 2, 2, 2), ("y_lo", "x", "z_hi", "z_lo", "core", "feat")
    )
    rows = ("y_lo", "x", "z_hi", "z_lo", "core")
    return jax.shard_map(
        layer,
        mesh=split,
        in_specs=(P(rows, "feat"), P(rows, "feat"), P(), P(), P(), P()),
        out_specs=(P(rows, "feat"), P(rows, "feat")),
        check_vma=False,
    )
```

```python
import math

import jax
import jax.numpy as jnp
from jax import lax
from jax.experimental import pallas as pl
from jax.experimental.pallas import tpu as pltpu
from jax.sharding import Mesh
from jax.sharding import PartitionSpec as P

E = 192
HEADS = 6
HD = 32
GROUPS = 4
FEATS = 8
TRAIN_ROWS = 64
TEST_ROWS = 32
ROWS = TRAIN_ROWS + TEST_ROWS
SIDE = 4
LANES = 128
REST = E - LANES
TRAIN_PACK = TRAIN_ROWS + TRAIN_ROWS // 2
PACK = ROWS + ROWS // 2
OWN_Q = GROUPS * ROWS
ALL_Q = 2 * OWN_Q
SOURCES = GROUPS * SIDE
KEYS = SOURCES * TRAIN_ROWS
SUMS = HD + 16
FOLD = E + 16
PROBES = 64
BLOCK = SOURCES * TRAIN_PACK
STATE = HD + 8

eps_norm = 1e-05
far_below = -3e38
safe_size = 2.0**60
log2_scale = HD ** (-0.5) * math.log2(math.e)


bf16 = jnp.bfloat16
f32 = jnp.float32


def mm(left, right):
    return jnp.dot(left, right, preferred_element_type=f32)


def mm_nt(left, right):
    return lax.dot_general(left, right, (((1,), (1,)), ((), ())), preferred_element_type=f32)


def layer_norm(values_in):
    centred = values_in - jnp.mean(values_in, axis=-1, keepdims=True)
    spread = jnp.mean(centred * centred, axis=-1, keepdims=True)
    return centred * lax.rsqrt(spread + eps_norm)


def call(kernel, outs, args, flops, scratch=(), limit=12):
    in_vmem = pl.BlockSpec(memory_space=pltpu.VMEM)
    return pl.pallas_call(
        kernel,
        out_shape=outs,
        in_specs=[in_vmem] * len(args),
        out_specs=[in_vmem] * len(outs),
        scratch_shapes=list(scratch),
        compiler_params=pltpu.CompilerParams(vmem_limit_bytes=limit * 2**20),
        cost_estimate=pl.CostEstimate(flops=flops, transcendentals=0, bytes_accessed=2**20),
    )(*args)


def pack_rows(rows):
    half = rows.shape[0] // 2
    rest = rows[:, LANES:]
    return [rows[:, :LANES], jnp.concatenate([rest[:half], rest[half:]], axis=1)]


def pack(rows):
    parts = pack_rows(rows[:TRAIN_ROWS]) + pack_rows(rows[TRAIN_ROWS:])
    return jnp.concatenate(parts, axis=0).astype(bf16)


def unpack_rows(packed):
    height = packed.shape[0] * 2 // 3
    rest = packed[height:]
    rest = jnp.concatenate([rest[:, :REST], rest[:, REST:]], axis=0)
    return jnp.concatenate([packed[:height], rest], axis=1)


def unpack(packed):
    packed = packed.astype(f32)
    parts = [unpack_rows(packed[:TRAIN_PACK]), unpack_rows(packed[TRAIN_PACK:])]
    return jnp.concatenate(parts, axis=0)


def near_kernel(train_ref, test_ref, weights_ref, cells_ref, query_ref, key_ref, value_ref):
    parts = []
    for index in range(GROUPS):
        span = slice(index * E, (index + 1) * E)
        cell = [one_ref[:, span].astype(f32) for one_ref in (train_ref, test_ref)]
        cell = jnp.concatenate(cell, axis=0)
        cells_ref[index] = cell
        parts.append(layer_norm(cell).astype(bf16))
    normed = jnp.concatenate(parts, axis=0)
    query_ref[...] = (mm(normed, weights_ref[0]) * log2_scale).astype(bf16)
    key_ref[...] = mm(normed, weights_ref[1]).astype(bf16)
    value_ref[...] = mm(normed, weights_ref[2]).astype(bf16)


def before_kernel(
    other_ref, weights_ref, cells_ref, query_ref, key_ref, value_ref, after_ref, send_ref
):
    parts = []
    for index in range(GROUPS):
        cell = other_ref[:, index * E : (index + 1) * E].astype(f32)
        parts.append(layer_norm(cell).astype(bf16))
    normed = jnp.concatenate(parts, axis=0)
    far_keys = mm(normed, weights_ref[1]).astype(bf16)
    far_values = mm(normed, weights_ref[2]).astype(bf16)
    queries = query_ref[...]
    keys = jnp.concatenate([key_ref[...], far_keys], axis=0)
    values = jnp.concatenate([value_ref[...], far_values], axis=0).astype(f32)
    head_of = lax.broadcasted_iota(jnp.int32, (E, 128), 0) >> 5
    gather = jnp.where(head_of == lax.broadcasted_iota(jnp.int32, (E, 128), 1), 1.0, 0.0).astype(bf16)
    head_to = lax.broadcasted_iota(jnp.int32, (128, E), 1) >> 5
    spread = jnp.where(head_to == lax.broadcasted_iota(jnp.int32, (128, E), 0), 1.0, 0.0).astype(bf16)
    mixtures = []
    for index in range(GROUPS):
        asked = queries[index * ROWS : (index + 1) * ROWS]
        products = jnp.concatenate(
            [asked * keys[j * ROWS : (j + 1) * ROWS] for j in range(FEATS)], axis=0
        )
        scores = mm(products, gather)
        pieces = [scores[j * ROWS : (j + 1) * ROWS] for j in range(FEATS)]
        peak = pieces[0]
        for one in pieces[1:]:
            peak = jnp.maximum(peak, one)
        weights = [jnp.exp2(one - peak) for one in pieces]
        total = weights[0]
        for one in weights[1:]:
            total = total + one
        high = total.astype(bf16)
        low = (total - high.astype(f32)).astype(bf16)
        wide = mm(jnp.concatenate([one.astype(bf16) for one in weights] + [high, low], axis=0), spread)
        mixed = wide[:ROWS] * values[:ROWS]
        for j in range(1, FEATS):
            mixed = mixed + wide[j * ROWS : (j + 1) * ROWS] * values[j * ROWS : (j + 1) * ROWS]
        whole = wide[FEATS * ROWS : (FEATS + 1) * ROWS] + wide[(FEATS + 1) * ROWS :]
        mixtures.append((mixed / whole).astype(bf16))
    moved = mm(jnp.concatenate(mixtures, axis=0), weights_ref[3]).astype(bf16).astype(f32)
    for index in range(GROUPS):
        after = cells_ref[index] + moved[index * ROWS : (index + 1) * ROWS]
        after_ref[index] = after
        send_ref[index] = pack(layer_norm(after))


def fold_kernel(own_ref, other_ref, weights_ref, folded_ref, turned_ref):
    turned_ref[...] = weights_ref[2].astype(f32).T.astype(bf16)
    parts = [unpack(one_ref[index]) for one_ref in (own_ref, other_ref) for index in range(GROUPS)]
    asked = jnp.concatenate(parts, axis=0).astype(bf16)
    probes = jnp.concatenate([parts[0][:PROBES], parts[GROUPS][:PROBES]], axis=0).astype(bf16)
    queries = (mm(asked, weights_ref[0]) * log2_scale).astype(bf16)
    weight = weights_ref[1]
    row = lax.broadcasted_iota(jnp.int32, (FOLD - E, ALL_Q), 0)
    for head in range(HEADS):
        part = slice(head * HD, (head + 1) * HD)
        folded = mm_nt(weight[:, part], queries[:, part]).astype(bf16)
        peak = jnp.max(mm(probes, folded), axis=0, keepdims=True)
        folded_ref[head, :E, :] = folded
        folded_ref[head, E:, :] = jnp.where(row == 0, -peak, 0.0).astype(bf16)


def stack_kernel(upper_ref, lower_ref, both_ref):
    both_ref[: BLOCK // 4, :] = upper_ref[...]
    both_ref[BLOCK // 4 :, :] = lower_ref[...]


def stack(upper, lower):
    return call(
        stack_kernel,
        [jax.ShapeDtypeStruct((BLOCK // 2, LANES), bf16)],
        (upper, lower),
        10**6,
        limit=4,
    )[0]


def unpack_keys(packed_refs, keys_ref):
    half = TRAIN_ROWS // 2
    each = SOURCES // len(packed_refs)
    for source in range(SOURCES):
        packed_ref = packed_refs[source // each]
        low = source * TRAIN_ROWS
        top = source % each * TRAIN_PACK
        rest = packed_ref[top + TRAIN_ROWS : top + TRAIN_PACK, :]
        keys_ref[low : low + TRAIN_ROWS, :LANES] = packed_ref[top : top + TRAIN_ROWS, :]
        keys_ref[low : low + half, LANES:E] = rest[:, :REST]
        keys_ref[low + half : low + TRAIN_ROWS, LANES:E] = rest[:, REST:]
    keys_ref[:, E:] = jnp.ones((KEYS, FOLD - E), bf16)


def turn_values(wv_ref, keys_ref, values_ref):
    values = mm_nt(wv_ref[...], keys_ref[:, :E]).astype(bf16)
    for head in range(HEADS):
        values_ref[head, 0:HD, :] = values[head * HD : (head + 1) * HD, :]
        values_ref[head, HD:SUMS, :] = jnp.ones((SUMS - HD, KEYS), bf16)


def attend_kernel(first, packed_refs, refs):
    wv_ref, folded_ref = refs[:2]
    mix_out, keys_ref, values_ref = refs[-3:]
    unpack_keys(packed_refs, keys_ref)
    turn_values(wv_ref, keys_ref, values_ref)

    def work(head):
        weights = jnp.exp2(mm(keys_ref[...], folded_ref[head])).astype(bf16)
        mixed = mm(values_ref[head], weights)
        if not first:
            mixed = mixed + refs[2][head]
        mix_out[head] = mixed

    for head in range(HEADS):
        work(head)


def attend_last_kernel(*refs):
    packed_refs = refs[: 2 * SIDE]
    wv_ref, folded_ref, mix_ref, stay_ref, leave_ref = refs[2 * SIDE : 2 * SIDE + 5]
    keys_ref, values_ref, total_ref, peak_ref, blocks_ref, scores_ref = refs[2 * SIDE + 5 :]
    attend_kernel(
        False,
        packed_refs[:2],
        (wv_ref, folded_ref, mix_ref, total_ref, keys_ref, values_ref),
    )
    for head in range(HEADS):
        peak_ref[head] = -folded_ref[head, E:, :].astype(f32)[:8]
    over = jnp.where(jnp.abs(total_ref[...]) < safe_size, 0.0, 1.0)

    @pl.when(jnp.max(over) > 0.0)
    def _():
        for index, one_ref in enumerate(packed_refs):
            span = slice(index % 2 * BLOCK // 2, (index % 2 + 1) * BLOCK // 2)
            blocks_ref[index // 2, span] = one_ref[...]
        peak_ref[...] = jnp.full(peak_ref.shape, far_below, f32)
        total_ref[...] = jnp.zeros(total_ref.shape, f32)

        def one_block(index, carry):
            unpack_keys((blocks_ref.at[index],), keys_ref)
            turn_values(wv_ref, keys_ref, values_ref)

            def work(head, kept):
                scores_ref[...] = mm(keys_ref[:, :E], folded_ref[head, :E, :])
                old = peak_ref[head][0:1, :]
                peak = jnp.maximum(jnp.max(scores_ref[...], axis=0, keepdims=True), old)
                weights = jnp.exp2(scores_ref[...] - peak).astype(bf16)
                mixed = mm(values_ref[head], weights)
                total_ref[head] = total_ref[head] * jnp.exp2(old - peak) + mixed
                peak_ref[head] = jnp.broadcast_to(peak, (8, ALL_Q))
                return kept

            lax.fori_loop(0, HEADS, work, 0)
            return carry

        lax.fori_loop(0, SIDE, one_block, 0)

    for head in range(HEADS):
        total = total_ref[head]
        joined = jnp.concatenate(
            [total[: HD + 1], peak_ref[head][0:1, :], total[HD + 2 : STATE]], axis=0
        )
        stay_ref[head] = joined[:, :OWN_Q]
        leave_ref[head] = joined[:, OWN_Q:]


mix_shape = jax.ShapeDtypeStruct((HEADS, SUMS, ALL_Q), f32)
attend_scratch = [pltpu.VMEM((KEYS, FOLD), bf16), pltpu.VMEM((HEADS, SUMS, KEYS), bf16)]
attend_flops = 4 * HEADS * KEYS * ALL_Q * E


def attend(args):
    first = len(args) == 4
    return call(
        lambda *refs: attend_kernel(first, refs[:2], refs[2:]),
        [mix_shape],
        args,
        attend_flops,
        scratch=attend_scratch,
        limit=20,
    )[0]


def attend_last(args):
    return call(
        attend_last_kernel,
        [jax.ShapeDtypeStruct((HEADS, STATE, OWN_Q), f32)] * 2,
        args,
        attend_flops,
        scratch=attend_scratch
        + [
            pltpu.VMEM((HEADS, SUMS, ALL_Q), f32),
            pltpu.VMEM((HEADS, 8, ALL_Q), f32),
            pltpu.VMEM((SIDE, BLOCK, LANES), bf16),
            pltpu.VMEM((KEYS, ALL_Q), f32),
        ],
        limit=20,
    )


def merge_kernel(stay_ref, came_ref, send_ref):
    parts = []
    for head in range(HEADS):
        stay = stay_ref[head]
        came = came_ref[head]
        peak = jnp.maximum(stay[HD + 1 : HD + 2], came[HD + 1 : HD + 2])
        fade_stay = jnp.exp2(stay[HD + 1 : HD + 2] - peak)
        fade_came = jnp.exp2(came[HD + 1 : HD + 2] - peak)
        total = stay[HD : HD + 1] * fade_stay + came[HD : HD + 1] * fade_came
        mixed = stay[:HD] * fade_stay + came[:HD] * fade_came
        parts.append(mixed / total)
    turned = jnp.concatenate(parts, axis=0).T
    for peer in range(GROUPS):
        send_ref[peer] = pack(turned[peer * ROWS : (peer + 1) * ROWS])


def after_kernel(came_ref, after_ref, wo_ref, up_ref, down_ref, train_ref, test_ref):
    mixes = [unpack(came_ref[index]) for index in range(GROUPS)]
    row_mix = jnp.concatenate(mixes, axis=0).astype(bf16)
    after_row = after_ref[...].reshape(GROUPS * ROWS, E) + mm(row_mix, wo_ref[...])
    third = layer_norm(after_row).astype(bf16)
    raised = mm(third, up_ref[...])
    hidden = (0.5 * raised * (1.0 + lax.erf(raised * (0.5**0.5)))).astype(bf16)
    result = (after_row + mm(hidden, down_ref[...])).astype(bf16)
    for index in range(GROUPS):
        low = index * ROWS
        left = index * E
        train_ref[:, left : left + E] = result[low : low + TRAIN_ROWS]
        test_ref[:, left : left + E] = result[low + TRAIN_ROWS : low + ROWS]


def shift(size, by):
    return [(index, (index + by) % size) for index in range(size)]


def layer(train_cells, test_cells, feat_weights, row_weights, mlp_up, mlp_down):
    swap = [(0, 1), (1, 0)]
    joined = jnp.concatenate([train_cells, test_cells], axis=0)
    other = lax.ppermute(joined, "feat", swap)
    wide = (GROUPS * ROWS, E)
    near = call(
        near_kernel,
        [jax.ShapeDtypeStruct((GROUPS, ROWS, E), f32)] + [jax.ShapeDtypeStruct(wide, bf16)] * 3,
        (train_cells, test_cells, feat_weights),
        10**9,
    )
    after_feat, pieces = call(
        before_kernel,
        [
            jax.ShapeDtypeStruct((GROUPS, ROWS, E), f32),
            jax.ShapeDtypeStruct((GROUPS, PACK, LANES), bf16),
        ],
        (other, feat_weights, *near),
        10**9,
    )
    classes = ("y_lo", "z_lo")
    received = lax.all_to_all(pieces, classes, split_axis=0, concat_axis=0, tiled=True)
    keys = received[:, :TRAIN_PACK].reshape(GROUPS * TRAIN_PACK, LANES)
    column = [keys]
    for by in (1, 3, 2):
        column.append(lax.ppermute(keys, "z_hi", shift(SIDE, by)))
    received_other = lax.ppermute(received, "core", swap)
    early = stack(*column[:2])
    early_above = lax.ppermute(early, "x", shift(4, 1))
    early_below = lax.ppermute(early, "x", shift(4, 3))
    folded, value_turned = call(
        fold_kernel,
        [
            jax.ShapeDtypeStruct((HEADS, FOLD, ALL_Q), bf16),
            jax.ShapeDtypeStruct((E, E), bf16),
        ],
        (received, received_other, row_weights),
        10**9,
    )
    column, folded = lax.optimization_barrier((column[2:], folded))
    late = stack(*column)
    late_above = lax.ppermute(late, "x", shift(4, 1))
    late_below = lax.ppermute(late, "x", shift(4, 3))
    mix = attend((early, late, value_turned, folded))
    mix, early_above, late_below = lax.optimization_barrier((mix, early_above, late_below))
    far_early = lax.ppermute(early_above, "x", shift(4, 1))
    far_late = lax.ppermute(late_below, "x", shift(4, 3))
    mix = attend((early_above, early_below, value_turned, folded, mix))
    mix = attend((late_above, late_below, value_turned, folded, mix))
    packed = (far_early, far_late, early, late, early_above, early_below, late_above, late_below)
    stay, leave = attend_last(packed + (value_turned, folded, mix))
    came = lax.ppermute(leave, "core", swap)
    mixed = call(
        merge_kernel, [jax.ShapeDtypeStruct((GROUPS, PACK, LANES), bf16)], (stay, came), 10**7
    )[0]
    returned = lax.all_to_all(mixed, classes, split_axis=0, concat_axis=0, tiled=True)
    train_out, test_out = call(
        after_kernel,
        [
            jax.ShapeDtypeStruct((TRAIN_ROWS, GROUPS * E), bf16),
            jax.ShapeDtypeStruct((TEST_ROWS, GROUPS * E), bf16),
        ],
        (returned, after_feat, row_weights[3], mlp_up, mlp_down),
        10**9,
    )
    return (train_out, test_out)


def solution(mesh):
    split = Mesh(
        mesh.devices.reshape(2, 4, 4, 2, 2, 2), ("y_lo", "x", "z_hi", "z_lo", "core", "feat")
    )
    rows = ("y_lo", "x", "z_hi", "z_lo", "core")
    return jax.shard_map(
        layer,
        mesh=split,
        in_specs=(P(rows, "feat"), P(rows, "feat"), P(), P(), P(), P()),
        out_specs=(P(rows, "feat"), P(rows, "feat")),
        check_vma=False,
    )
```

```python
import math

import jax
import jax.numpy as jnp
from jax import lax
from jax.experimental import pallas as pl
from jax.experimental.pallas import tpu as pltpu
from jax.sharding import Mesh
from jax.sharding import PartitionSpec as P

E = 192
HEADS = 6
HD = 32
GROUPS = 4
FEATS = 8
TRAIN_ROWS = 64
TEST_ROWS = 32
ROWS = TRAIN_ROWS + TEST_ROWS
SIDE = 4
LANES = 128
REST = E - LANES
TRAIN_PACK = TRAIN_ROWS + TRAIN_ROWS // 2
PACK = ROWS + ROWS // 2
OWN_Q = GROUPS * ROWS
ALL_Q = 2 * OWN_Q
SOURCES = GROUPS * SIDE
KEYS = SOURCES * TRAIN_ROWS
SUMS = HD + 16
FOLD = E + 16
PROBES = 64
BLOCK = SOURCES * TRAIN_PACK
STATE = HD + 8

eps_norm = 1e-05
far_below = -3e38
safe_size = 2.0**60
log2_scale = HD ** (-0.5) * math.log2(math.e)


bf16 = jnp.bfloat16
f32 = jnp.float32


classes = ("y_lo", "z_lo")
piece_shape = jax.ShapeDtypeStruct((PACK, LANES), bf16)


def mm(left, right):
    return jnp.dot(left, right, preferred_element_type=f32)


def mm_nt(left, right):
    return lax.dot_general(left, right, (((1,), (1,)), ((), ())), preferred_element_type=f32)


def layer_norm(values_in):
    centred = values_in - jnp.mean(values_in, axis=-1, keepdims=True)
    spread = jnp.mean(centred * centred, axis=-1, keepdims=True)
    return centred * lax.rsqrt(spread + eps_norm)


def call(kernel, outs, args, flops, scratch=(), limit=12):
    in_vmem = pl.BlockSpec(memory_space=pltpu.VMEM)
    return pl.pallas_call(
        kernel,
        out_shape=outs,
        in_specs=[in_vmem] * len(args),
        out_specs=[in_vmem] * len(outs),
        scratch_shapes=list(scratch),
        compiler_params=pltpu.CompilerParams(vmem_limit_bytes=limit * 2**20),
        cost_estimate=pl.CostEstimate(flops=flops, transcendentals=0, bytes_accessed=2**20),
    )(*args)


def pack_rows(rows):
    half = rows.shape[0] // 2
    rest = rows[:, LANES:]
    return [rows[:, :LANES], jnp.concatenate([rest[:half], rest[half:]], axis=1)]


def pack(rows):
    parts = pack_rows(rows[:TRAIN_ROWS]) + pack_rows(rows[TRAIN_ROWS:])
    return jnp.concatenate(parts, axis=0).astype(bf16)


def unpack_rows(packed):
    height = packed.shape[0] * 2 // 3
    rest = packed[height:]
    rest = jnp.concatenate([rest[:, :REST], rest[:, REST:]], axis=0)
    return jnp.concatenate([packed[:height], rest], axis=1)


def unpack(packed):
    packed = packed.astype(f32)
    parts = [unpack_rows(packed[:TRAIN_PACK]), unpack_rows(packed[TRAIN_PACK:])]
    return jnp.concatenate(parts, axis=0)


def near_kernel(train_ref, test_ref, weights_ref, cells_ref, query_ref, key_ref, value_ref):
    parts = []
    for index in range(GROUPS):
        span = slice(index * E, (index + 1) * E)
        cell = [one_ref[:, span].astype(f32) for one_ref in (train_ref, test_ref)]
        cell = jnp.concatenate(cell, axis=0)
        cells_ref[index] = cell
        parts.append(layer_norm(cell).astype(bf16))
    normed = jnp.concatenate(parts, axis=0)
    query_ref[...] = (mm(normed, weights_ref[0]) * log2_scale).astype(bf16)
    key_ref[...] = mm(normed, weights_ref[1]).astype(bf16)
    value_ref[...] = mm(normed, weights_ref[2]).astype(bf16)


def own_class():
    return lax.axis_index(classes)


def before_kernel(
    other_ref, weights_ref, cells_ref, query_ref, key_ref, value_ref, after_ref, *refs
):
    send_refs, pieces_ref = refs[:GROUPS], refs[GROUPS]
    parts = []
    for index in range(GROUPS):
        cell = other_ref[:, index * E : (index + 1) * E].astype(f32)
        parts.append(layer_norm(cell).astype(bf16))
    normed = jnp.concatenate(parts, axis=0)
    far_keys = mm(normed, weights_ref[1]).astype(bf16)
    far_values = mm(normed, weights_ref[2]).astype(bf16)
    queries = query_ref[...]
    keys = jnp.concatenate([key_ref[...], far_keys], axis=0)
    values = jnp.concatenate([value_ref[...], far_values], axis=0).astype(f32)
    head_of = lax.broadcasted_iota(jnp.int32, (E, 128), 0) >> 5
    gather = jnp.where(head_of == lax.broadcasted_iota(jnp.int32, (E, 128), 1), 1.0, 0.0).astype(bf16)
    head_to = lax.broadcasted_iota(jnp.int32, (128, E), 1) >> 5
    spread = jnp.where(head_to == lax.broadcasted_iota(jnp.int32, (128, E), 0), 1.0, 0.0).astype(bf16)
    mixtures = []
    for index in range(GROUPS):
        asked = queries[index * ROWS : (index + 1) * ROWS]
        products = jnp.concatenate(
            [asked * keys[j * ROWS : (j + 1) * ROWS] for j in range(FEATS)], axis=0
        )
        scores = mm(products, gather)
        pieces = [scores[j * ROWS : (j + 1) * ROWS] for j in range(FEATS)]
        peak = pieces[0]
        for one in pieces[1:]:
            peak = jnp.maximum(peak, one)
        weights = [jnp.exp2(one - peak) for one in pieces]
        total = weights[0]
        for one in weights[1:]:
            total = total + one
        high = total.astype(bf16)
        low = (total - high.astype(f32)).astype(bf16)
        wide = mm(jnp.concatenate([one.astype(bf16) for one in weights] + [high, low], axis=0), spread)
        mixed = wide[:ROWS] * values[:ROWS]
        for j in range(1, FEATS):
            mixed = mixed + wide[j * ROWS : (j + 1) * ROWS] * values[j * ROWS : (j + 1) * ROWS]
        whole = wide[FEATS * ROWS : (FEATS + 1) * ROWS] + wide[(FEATS + 1) * ROWS :]
        mixtures.append((mixed / whole).astype(bf16))
    moved = mm(jnp.concatenate(mixtures, axis=0), weights_ref[3]).astype(bf16).astype(f32)
    for index in range(GROUPS):
        after = cells_ref[index] + moved[index * ROWS : (index + 1) * ROWS]
        after_ref[index] = after
        pieces_ref[index] = pack(layer_norm(after))
    for turn in range(GROUPS):
        send_refs[turn][...] = pieces_ref[own_class() ^ turn]


def gather_kernel(*refs):
    received_ref, keys_ref = refs[GROUPS:]
    for turn in range(GROUPS):
        piece = refs[turn][...]
        received_ref[turn] = piece
        keys_ref[turn * TRAIN_PACK : (turn + 1) * TRAIN_PACK, :] = piece[:TRAIN_PACK]


def exchange(pieces):
    came = [pieces[0]]
    for turn in range(1, GROUPS):
        pairs = [(one, one ^ turn) for one in range(GROUPS)]
        came.append(lax.ppermute(pieces[turn], classes, pairs))
    return came


def fold_kernel(own_ref, other_ref, weights_ref, folded_ref, turned_ref):
    turned_ref[...] = weights_ref[2].astype(f32).T.astype(bf16)
    parts = [unpack(one_ref[index]) for one_ref in (own_ref, other_ref) for index in range(GROUPS)]
    asked = jnp.concatenate(parts, axis=0).astype(bf16)
    probes = jnp.concatenate([parts[0][:PROBES], parts[GROUPS][:PROBES]], axis=0).astype(bf16)
    queries = (mm(asked, weights_ref[0]) * log2_scale).astype(bf16)
    weight = weights_ref[1]
    row = lax.broadcasted_iota(jnp.int32, (FOLD - E, ALL_Q), 0)
    for head in range(HEADS):
        part = slice(head * HD, (head + 1) * HD)
        folded = mm_nt(weight[:, part], queries[:, part]).astype(bf16)
        peak = jnp.max(mm(probes, folded), axis=0, keepdims=True)
        folded_ref[head, :E, :] = folded
        folded_ref[head, E:, :] = jnp.where(row == 0, -peak, 0.0).astype(bf16)


def stack_kernel(upper_ref, lower_ref, both_ref):
    both_ref[: BLOCK // 4, :] = upper_ref[...]
    both_ref[BLOCK // 4 :, :] = lower_ref[...]


def stack(upper, lower):
    return call(
        stack_kernel,
        [jax.ShapeDtypeStruct((BLOCK // 2, LANES), bf16)],
        (upper, lower),
        10**6,
        limit=4,
    )[0]


def unpack_keys(packed_refs, keys_ref):
    half = TRAIN_ROWS // 2
    each = SOURCES // len(packed_refs)
    for source in range(SOURCES):
        packed_ref = packed_refs[source // each]
        low = source * TRAIN_ROWS
        top = source % each * TRAIN_PACK
        rest = packed_ref[top + TRAIN_ROWS : top + TRAIN_PACK, :]
        keys_ref[low : low + TRAIN_ROWS, :LANES] = packed_ref[top : top + TRAIN_ROWS, :]
        keys_ref[low : low + half, LANES:E] = rest[:, :REST]
        keys_ref[low + half : low + TRAIN_ROWS, LANES:E] = rest[:, REST:]
    keys_ref[:, E:] = jnp.ones((KEYS, FOLD - E), bf16)


def turn_values(wv_ref, keys_ref, values_ref):
    values = mm_nt(wv_ref[...], keys_ref[:, :E]).astype(bf16)
    for head in range(HEADS):
        values_ref[head, 0:HD, :] = values[head * HD : (head + 1) * HD, :]
        values_ref[head, HD:SUMS, :] = jnp.ones((SUMS - HD, KEYS), bf16)


def attend_kernel(first, packed_refs, refs):
    wv_ref, folded_ref = refs[:2]
    mix_out, keys_ref, values_ref = refs[-3:]
    unpack_keys(packed_refs, keys_ref)
    turn_values(wv_ref, keys_ref, values_ref)

    def work(head):
        weights = jnp.exp2(mm(keys_ref[...], folded_ref[head])).astype(bf16)
        mixed = mm(values_ref[head], weights)
        if not first:
            mixed = mixed + refs[2][head]
        mix_out[head] = mixed

    for head in range(HEADS):
        work(head)


def attend_last_kernel(*refs):
    packed_refs = refs[: 2 * SIDE]
    wv_ref, folded_ref, mix_ref, stay_ref, leave_ref = refs[2 * SIDE : 2 * SIDE + 5]
    keys_ref, values_ref, total_ref, peak_ref, blocks_ref, scores_ref = refs[2 * SIDE + 5 :]
    attend_kernel(
        False,
        packed_refs[:2],
        (wv_ref, folded_ref, mix_ref, total_ref, keys_ref, values_ref),
    )
    for head in range(HEADS):
        peak_ref[head] = -folded_ref[head, E:, :].astype(f32)[:8]
    over = jnp.where(jnp.abs(total_ref[...]) < safe_size, 0.0, 1.0)

    @pl.when(jnp.max(over) > 0.0)
    def _():
        for index, one_ref in enumerate(packed_refs):
            span = slice(index % 2 * BLOCK // 2, (index % 2 + 1) * BLOCK // 2)
            blocks_ref[index // 2, span] = one_ref[...]
        peak_ref[...] = jnp.full(peak_ref.shape, far_below, f32)
        total_ref[...] = jnp.zeros(total_ref.shape, f32)

        def one_block(index, carry):
            unpack_keys((blocks_ref.at[index],), keys_ref)
            turn_values(wv_ref, keys_ref, values_ref)

            def work(head, kept):
                scores_ref[...] = mm(keys_ref[:, :E], folded_ref[head, :E, :])
                old = peak_ref[head][0:1, :]
                peak = jnp.maximum(jnp.max(scores_ref[...], axis=0, keepdims=True), old)
                weights = jnp.exp2(scores_ref[...] - peak).astype(bf16)
                mixed = mm(values_ref[head], weights)
                total_ref[head] = total_ref[head] * jnp.exp2(old - peak) + mixed
                peak_ref[head] = jnp.broadcast_to(peak, (8, ALL_Q))
                return kept

            lax.fori_loop(0, HEADS, work, 0)
            return carry

        lax.fori_loop(0, SIDE, one_block, 0)

    for head in range(HEADS):
        total = total_ref[head]
        joined = jnp.concatenate(
            [total[: HD + 1], peak_ref[head][0:1, :], total[HD + 2 : STATE]], axis=0
        )
        stay_ref[head] = joined[:, :OWN_Q]
        leave_ref[head] = joined[:, OWN_Q:]


mix_shape = jax.ShapeDtypeStruct((HEADS, SUMS, ALL_Q), f32)
attend_scratch = [pltpu.VMEM((KEYS, FOLD), bf16), pltpu.VMEM((HEADS, SUMS, KEYS), bf16)]
attend_flops = 4 * HEADS * KEYS * ALL_Q * E


def attend(args):
    first = len(args) == 4
    return call(
        lambda *refs: attend_kernel(first, refs[:2], refs[2:]),
        [mix_shape],
        args,
        attend_flops,
        scratch=attend_scratch,
        limit=20,
    )[0]


def attend_last(args):
    return call(
        attend_last_kernel,
        [jax.ShapeDtypeStruct((HEADS, STATE, OWN_Q), f32)] * 2,
        args,
        attend_flops,
        scratch=attend_scratch
        + [
            pltpu.VMEM((HEADS, SUMS, ALL_Q), f32),
            pltpu.VMEM((HEADS, 8, ALL_Q), f32),
            pltpu.VMEM((SIDE, BLOCK, LANES), bf16),
            pltpu.VMEM((KEYS, ALL_Q), f32),
        ],
        limit=20,
    )


def merge_kernel(stay_ref, came_ref, *send_refs):
    parts = []
    for head in range(HEADS):
        stay = stay_ref[head]
        came = came_ref[head]
        peak = jnp.maximum(stay[HD + 1 : HD + 2], came[HD + 1 : HD + 2])
        fade_stay = jnp.exp2(stay[HD + 1 : HD + 2] - peak)
        fade_came = jnp.exp2(came[HD + 1 : HD + 2] - peak)
        total = stay[HD : HD + 1] * fade_stay + came[HD : HD + 1] * fade_came
        mixed = stay[:HD] * fade_stay + came[:HD] * fade_came
        parts.append(mixed / total)
    turned = jnp.concatenate(parts, axis=0).T
    for peer in range(GROUPS):
        send_refs[peer][...] = pack(turned[peer * ROWS : (peer + 1) * ROWS])


def after_kernel(*refs):
    came_refs = refs[:GROUPS]
    after_ref, wo_ref, up_ref, down_ref, train_ref, test_ref, pieces_ref = refs[GROUPS:]
    for turn in range(GROUPS):
        pieces_ref[own_class() ^ turn] = came_refs[turn][...]
    mixes = [unpack(pieces_ref[index]) for index in range(GROUPS)]
    row_mix = jnp.concatenate(mixes, axis=0).astype(bf16)
    after_row = after_ref[...].reshape(GROUPS * ROWS, E) + mm(row_mix, wo_ref[...])
    third = layer_norm(after_row).astype(bf16)
    raised = mm(third, up_ref[...])
    hidden = (0.5 * raised * (1.0 + lax.erf(raised * (0.5**0.5)))).astype(bf16)
    result = (after_row + mm(hidden, down_ref[...])).astype(bf16)
    for index in range(GROUPS):
        low = index * ROWS
        left = index * E
        train_ref[:, left : left + E] = result[low : low + TRAIN_ROWS]
        test_ref[:, left : left + E] = result[low + TRAIN_ROWS : low + ROWS]


def shift(size, by):
    return [(index, (index + by) % size) for index in range(size)]


def layer(train_cells, test_cells, feat_weights, row_weights, mlp_up, mlp_down):
    swap = [(0, 1), (1, 0)]
    joined = jnp.concatenate([train_cells, test_cells], axis=0)
    other = lax.ppermute(joined, "feat", swap)
    wide = (GROUPS * ROWS, E)
    near = call(
        near_kernel,
        [jax.ShapeDtypeStruct((GROUPS, ROWS, E), f32)] + [jax.ShapeDtypeStruct(wide, bf16)] * 3,
        (train_cells, test_cells, feat_weights),
        10**9,
    )
    after_feat, *pieces = call(
        before_kernel,
        [jax.ShapeDtypeStruct((GROUPS, ROWS, E), f32)] + [piece_shape] * GROUPS,
        (other, feat_weights, *near),
        10**9,
        scratch=[pltpu.VMEM((GROUPS, PACK, LANES), bf16)],
    )
    received, keys = call(
        gather_kernel,
        [
            jax.ShapeDtypeStruct((GROUPS, PACK, LANES), bf16),
            jax.ShapeDtypeStruct((GROUPS * TRAIN_PACK, LANES), bf16),
        ],
        exchange(pieces),
        10**6,
        limit=4,
    )
    column = [keys]
    for by in (1, 3, 2):
        column.append(lax.ppermute(keys, "z_hi", shift(SIDE, by)))
    received_other = lax.ppermute(received, "core", swap)
    early = stack(*column[:2])
    early_above = lax.ppermute(early, "x", shift(4, 1))
    early_below = lax.ppermute(early, "x", shift(4, 3))
    folded, value_turned = call(
        fold_kernel,
        [
            jax.ShapeDtypeStruct((HEADS, FOLD, ALL_Q), bf16),
            jax.ShapeDtypeStruct((E, E), bf16),
        ],
        (received, received_other, row_weights),
        10**9,
    )
    column, folded = lax.optimization_barrier((column[2:], folded))
    late = stack(*column)
    late_above = lax.ppermute(late, "x", shift(4, 1))
    late_below = lax.ppermute(late, "x", shift(4, 3))
    mix = attend((early, late, value_turned, folded))
    mix, early_above, late_below = lax.optimization_barrier((mix, early_above, late_below))
    far_early = lax.ppermute(early_above, "x", shift(4, 1))
    far_late = lax.ppermute(late_below, "x", shift(4, 3))
    mix = attend((early_above, early_below, value_turned, folded, mix))
    mix = attend((late_above, late_below, value_turned, folded, mix))
    packed = (far_early, far_late, early, late, early_above, early_below, late_above, late_below)
    stay, leave = attend_last(packed + (value_turned, folded, mix))
    came = lax.ppermute(leave, "core", swap)
    mixed = call(merge_kernel, [piece_shape] * GROUPS, (stay, came), 10**7)
    train_out, test_out = call(
        after_kernel,
        [
            jax.ShapeDtypeStruct((TRAIN_ROWS, GROUPS * E), bf16),
            jax.ShapeDtypeStruct((TEST_ROWS, GROUPS * E), bf16),
        ],
        (*exchange(mixed), after_feat, row_weights[3], mlp_up, mlp_down),
        10**9,
        scratch=[pltpu.VMEM((GROUPS, PACK, LANES), bf16)],
    )
    return (train_out, test_out)


def solution(mesh):
    split = Mesh(
        mesh.devices.reshape(2, 4, 4, 2, 2, 2), ("y_lo", "x", "z_hi", "z_lo", "core", "feat")
    )
    rows = ("y_lo", "x", "z_hi", "z_lo", "core")
    return jax.shard_map(
        layer,
        mesh=split,
        in_specs=(P(rows, "feat"), P(rows, "feat"), P(), P(), P(), P()),
        out_specs=(P(rows, "feat"), P(rows, "feat")),
        check_vma=False,
    )
```

```python
import math

import jax
import jax.numpy as jnp
from jax import lax
from jax.experimental import pallas as pl
from jax.experimental.pallas import tpu as pltpu
from jax.sharding import Mesh
from jax.sharding import PartitionSpec as P

E = 192
HEADS = 6
HD = 32
GROUPS = 4
TRAIN_ROWS = 64
TEST_ROWS = 32
ROWS = TRAIN_ROWS + TEST_ROWS
SIDE = 4
LANES = 128
REST = E - LANES
TRAIN_PACK = TRAIN_ROWS + TRAIN_ROWS // 2
PACK = ROWS + ROWS // 2
OWN_Q = GROUPS * ROWS
ALL_Q = 2 * OWN_Q
SOURCES = GROUPS * SIDE
KEYS = SOURCES * TRAIN_ROWS
SUMS = HD + 16
FOLD = E + 16
PROBES = 16
KEY_STEP = 256
AHEAD = 2
BLOCK = SOURCES * TRAIN_PACK
STATE = HD + 8

eps_norm = 1e-05
far_below = -3e38
safe_size = 2.0**60
log2_scale = HD ** (-0.5) * math.log2(math.e)


bf16 = jnp.bfloat16
f32 = jnp.float32


classes = ("y_lo", "z_lo")
piece_shape = jax.ShapeDtypeStruct((PACK, LANES), bf16)


def mm(left, right):
    return jnp.dot(left, right, preferred_element_type=f32)


def mm_nt(left, right):
    return lax.dot_general(left, right, (((1,), (1,)), ((), ())), preferred_element_type=f32)


def layer_norm(values_in):
    centred = values_in - jnp.mean(values_in, axis=-1, keepdims=True)
    spread = jnp.mean(centred * centred, axis=-1, keepdims=True)
    return centred * lax.rsqrt(spread + eps_norm)


def call(kernel, outs, args, flops, scratch=(), limit=12):
    in_vmem = pl.BlockSpec(memory_space=pltpu.VMEM)
    return pl.pallas_call(
        kernel,
        out_shape=outs,
        in_specs=[in_vmem] * len(args),
        out_specs=[in_vmem] * len(outs),
        scratch_shapes=list(scratch),
        compiler_params=pltpu.CompilerParams(vmem_limit_bytes=limit * 2**20),
        cost_estimate=pl.CostEstimate(flops=flops, transcendentals=0, bytes_accessed=2**20),
    )(*args)


def pack_rows(rows):
    half = rows.shape[0] // 2
    rest = rows[:, LANES:]
    return [rows[:, :LANES], jnp.concatenate([rest[:half], rest[half:]], axis=1)]


def pack(rows):
    parts = pack_rows(rows[:TRAIN_ROWS]) + pack_rows(rows[TRAIN_ROWS:])
    return jnp.concatenate(parts, axis=0).astype(bf16)


def unpack_rows(packed):
    height = packed.shape[0] * 2 // 3
    rest = packed[height:]
    rest = jnp.concatenate([rest[:, :REST], rest[:, REST:]], axis=0)
    return jnp.concatenate([packed[:height], rest], axis=1)


def unpack(packed):
    packed = packed.astype(f32)
    parts = [unpack_rows(packed[:TRAIN_PACK]), unpack_rows(packed[TRAIN_PACK:])]
    return jnp.concatenate(parts, axis=0)


def head_maps():
    head_of = lax.broadcasted_iota(jnp.int32, (E, 128), 0) >> 5
    head_in = lax.broadcasted_iota(jnp.int32, (E, 128), 1)
    head_to = lax.broadcasted_iota(jnp.int32, (128, E), 1) >> 5
    head_out = lax.broadcasted_iota(jnp.int32, (128, E), 0)
    gather = jnp.where(head_of == head_in, 1.0, 0.0).astype(bf16)
    return gather, jnp.where(head_to == head_out, 1.0, 0.0).astype(bf16)


def rows_of(table, index):
    return table[index * ROWS : (index + 1) * ROWS]


def group_scores(asked, keys, gather):
    products = [asked * rows_of(keys, j) for j in range(GROUPS)]
    scores = mm(jnp.concatenate(products, axis=0), gather)
    return [rows_of(scores, j) for j in range(GROUPS)]


def halves(total):
    high = total.astype(bf16)
    return [high, (total - high.astype(f32)).astype(bf16)]


def near_kernel(
    train_ref,
    test_ref,
    weights_ref,
    cells_ref,
    query_ref,
    peak_ref,
    total_ref,
    mixed_ref,
):
    parts = []
    for index in range(GROUPS):
        span = slice(index * E, (index + 1) * E)
        cell = [one_ref[:, span].astype(f32) for one_ref in (train_ref, test_ref)]
        cell = jnp.concatenate(cell, axis=0)
        cells_ref[index] = cell
        parts.append(layer_norm(cell).astype(bf16))
    normed = jnp.concatenate(parts, axis=0)
    queries = (mm(normed, weights_ref[0]) * log2_scale).astype(bf16)
    query_ref[...] = queries
    keys = mm(normed, weights_ref[1]).astype(bf16)
    values = mm(normed, weights_ref[2]).astype(bf16).astype(f32)
    gather, spread = head_maps()
    for index in range(GROUPS):
        scores = group_scores(rows_of(queries, index), keys, gather)
        peak = scores[0]
        for one in scores[1:]:
            peak = jnp.maximum(peak, one)
        weights = [jnp.exp2(one - peak) for one in scores]
        total = weights[0]
        for one in weights[1:]:
            total = total + one
        wide = mm(jnp.concatenate([one.astype(bf16) for one in weights], axis=0), spread)
        mixed = rows_of(wide, 0) * rows_of(values, 0)
        for j in range(1, GROUPS):
            mixed = mixed + rows_of(wide, j) * rows_of(values, j)
        peak_ref[index] = peak
        total_ref[index] = total
        mixed_ref[index] = mixed


def own_class():
    return lax.axis_index(classes)


def before_kernel(
    other_ref, weights_ref, cells_ref, query_ref, peak_ref, total_ref, mixed_ref, after_ref, *refs
):
    send_refs, pieces_ref = refs[:GROUPS], refs[GROUPS]
    parts = []
    for index in range(GROUPS):
        cell = other_ref[:, index * E : (index + 1) * E].astype(f32)
        parts.append(layer_norm(cell).astype(bf16))
    normed = jnp.concatenate(parts, axis=0)
    keys = mm(normed, weights_ref[1]).astype(bf16)
    values = mm(normed, weights_ref[2]).astype(bf16).astype(f32)
    gather, spread = head_maps()
    mixtures = []
    for index in range(GROUPS):
        scores = group_scores(query_ref[index * ROWS : (index + 1) * ROWS, :], keys, gather)
        near_peak = peak_ref[index]
        peak = near_peak
        for one in scores:
            peak = jnp.maximum(peak, one)
        fade = jnp.exp2(near_peak - peak)
        weights = [jnp.exp2(one - peak) for one in scores]
        total = total_ref[index] * fade
        for one in weights:
            total = total + one
        widened = [one.astype(bf16) for one in weights] + halves(fade) + halves(total)
        wide = mm(jnp.concatenate(widened, axis=0), spread)
        mixed = mixed_ref[index] * (rows_of(wide, GROUPS) + rows_of(wide, GROUPS + 1))
        for j in range(GROUPS):
            mixed = mixed + rows_of(wide, j) * rows_of(values, j)
        whole = rows_of(wide, GROUPS + 2) + rows_of(wide, GROUPS + 3)
        mixtures.append((mixed / whole).astype(bf16))
    moved = mm(jnp.concatenate(mixtures, axis=0), weights_ref[3]).astype(bf16).astype(f32)
    for index in range(GROUPS):
        after = cells_ref[index] + moved[index * ROWS : (index + 1) * ROWS]
        after_ref[index] = after
        pieces_ref[index] = pack(layer_norm(after))
    for turn in range(GROUPS):
        send_refs[turn][...] = pieces_ref[own_class() ^ turn]


def gather_kernel(*refs):
    received_ref, keys_ref = refs[GROUPS:]
    for turn in range(GROUPS):
        piece = refs[turn][...]
        received_ref[turn] = piece
        keys_ref[turn * TRAIN_PACK : (turn + 1) * TRAIN_PACK, :] = piece[:TRAIN_PACK]


def exchange(pieces):
    came = [pieces[0]]
    for turn in range(1, GROUPS):
        pairs = [(one, one ^ turn) for one in range(GROUPS)]
        came.append(lax.ppermute(pieces[turn], classes, pairs))
    return came


def fold_kernel(own_ref, other_ref, weights_ref, folded_ref, turned_ref):
    turned_ref[...] = weights_ref[2].astype(f32).T.astype(bf16)
    parts = [unpack(one_ref[index]) for one_ref in (own_ref, other_ref) for index in range(GROUPS)]
    asked = jnp.concatenate(parts, axis=0).astype(bf16)
    probes = jnp.concatenate([parts[0][:PROBES], parts[GROUPS][:PROBES]], axis=0).astype(bf16)
    queries = (mm(asked, weights_ref[0]) * log2_scale).astype(bf16)
    weight = weights_ref[1]
    row = lax.broadcasted_iota(jnp.int32, (FOLD - E, ALL_Q), 0)
    for head in range(HEADS):
        part = slice(head * HD, (head + 1) * HD)
        folded = mm_nt(weight[:, part], queries[:, part]).astype(bf16)
        peak = jnp.max(mm(probes, folded), axis=0, keepdims=True)
        folded_ref[head, :E, :] = folded
        folded_ref[head, E:, :] = jnp.where(row == 0, -peak, 0.0).astype(bf16)


def stack_kernel(upper_ref, lower_ref, both_ref):
    both_ref[: BLOCK // 4, :] = upper_ref[...]
    both_ref[BLOCK // 4 :, :] = lower_ref[...]


def stack(upper, lower):
    return call(
        stack_kernel,
        [jax.ShapeDtypeStruct((BLOCK // 2, LANES), bf16)],
        (upper, lower),
        10**6,
        limit=4,
    )[0]


def unpack_keys(packed_refs, keys_ref):
    half = TRAIN_ROWS // 2
    each = SOURCES // 2
    for source in range(len(packed_refs) * each):
        packed_ref = packed_refs[source // each]
        low = source * TRAIN_ROWS
        top = source % each * TRAIN_PACK
        rest = packed_ref[top + TRAIN_ROWS : top + TRAIN_PACK, :]
        keys_ref[low : low + TRAIN_ROWS, :LANES] = packed_ref[top : top + TRAIN_ROWS, :]
        keys_ref[low : low + half, LANES:E] = rest[:, :REST]
        keys_ref[low + half : low + TRAIN_ROWS, LANES:E] = rest[:, REST:]
    keys_ref[:, E:] = jnp.ones((keys_ref.shape[0], FOLD - E), bf16)


def turn_values(wv_ref, keys_ref, values_ref):
    values = mm_nt(wv_ref[...], keys_ref[:, :E]).astype(bf16)
    for head in range(HEADS):
        values_ref[head, 0:HD, :] = values[head * HD : (head + 1) * HD, :]
        values_ref[head, HD:SUMS, :] = jnp.ones((SUMS - HD, keys_ref.shape[0]), bf16)


def attend_heads(packed_refs, wv_ref, folded_ref, keys_ref, values_ref, finish):
    unpack_keys(packed_refs, keys_ref)
    turn_values(wv_ref, keys_ref, values_ref)
    steps = keys_ref.shape[0] // KEY_STEP
    waiting = []
    sums = {}

    def drain():
        head, step, weights = waiting.pop(0)
        part = mm(values_ref[head, :, step * KEY_STEP : (step + 1) * KEY_STEP], weights)
        sums[head] = sums[head] + part if step else part
        if step == steps - 1:
            finish(head, sums.pop(head))

    for head in range(HEADS):
        for step in range(steps):
            scores = mm(keys_ref[step * KEY_STEP : (step + 1) * KEY_STEP, :], folded_ref[head])
            waiting.append((head, step, jnp.exp2(scores).astype(bf16)))
            if len(waiting) > AHEAD:
                drain()
    while waiting:
        drain()


def attend_kernel(first, packed_refs, refs):
    wv_ref, folded_ref = refs[:2]
    mix_out, keys_ref, values_ref = refs[-3:]

    def finish(head, mixed):
        mix_out[head] = mixed if first else mixed + refs[2][head]

    attend_heads(packed_refs, wv_ref, folded_ref, keys_ref, values_ref, finish)


def attend_last_kernel(*refs):
    packed_refs = refs[: 2 * SIDE]
    wv_ref, folded_ref, mix_ref, stay_ref, leave_ref = refs[2 * SIDE : 2 * SIDE + 5]
    keys_ref, values_ref, total_ref, peak_ref, blocks_ref, scores_ref = refs[2 * SIDE + 5 :]
    over = [jnp.zeros((8, ALL_Q), f32)]

    def leave(head, total, peak):
        joined = jnp.concatenate([total[: HD + 1], peak, total[HD + 2 : STATE]], axis=0)
        stay_ref[head] = joined[:, :OWN_Q]
        leave_ref[head] = joined[:, OWN_Q:]

    def finish(head, mixed):
        total = mixed + mix_ref[head]
        grown = jnp.where(jnp.abs(total) < safe_size, 0.0, 1.0)
        over[0] = jnp.maximum(over[0], jnp.max(grown.reshape(SUMS // 8, 8, ALL_Q), axis=0))
        leave(head, total, -folded_ref[head, E:, :].astype(f32)[:1])

    attend_heads(packed_refs[:2], wv_ref, folded_ref, keys_ref, values_ref, finish)

    @pl.when(jnp.max(over[0]) > 0.0)
    def _():
        for index, one_ref in enumerate(packed_refs):
            blocks_ref[index] = one_ref[...]
        peak_ref[...] = jnp.full(peak_ref.shape, far_below, f32)
        total_ref[...] = jnp.zeros(total_ref.shape, f32)

        def one_block(index, carry):
            unpack_keys((blocks_ref.at[2 * index], blocks_ref.at[2 * index + 1]), keys_ref)
            turn_values(wv_ref, keys_ref, values_ref)

            def work(head, kept):
                scores_ref[...] = mm(keys_ref[:, :E], folded_ref[head, :E, :])
                old = peak_ref[head][0:1, :]
                peak = jnp.maximum(jnp.max(scores_ref[...], axis=0, keepdims=True), old)
                weights = jnp.exp2(scores_ref[...] - peak).astype(bf16)
                mixed = mm(values_ref[head], weights)
                total_ref[head] = total_ref[head] * jnp.exp2(old - peak) + mixed
                peak_ref[head] = jnp.broadcast_to(peak, (8, ALL_Q))
                return kept

            lax.fori_loop(0, HEADS, work, 0)
            return carry

        lax.fori_loop(0, SIDE, one_block, 0)
        for head in range(HEADS):
            leave(head, total_ref[head], peak_ref[head][0:1, :])


mix_shape = jax.ShapeDtypeStruct((HEADS, SUMS, ALL_Q), f32)
attend_flops = 4 * HEADS * KEYS * ALL_Q * E


def attend_scratch(keys):
    return [pltpu.VMEM((keys, FOLD), bf16), pltpu.VMEM((HEADS, SUMS, keys), bf16)]


def attend(packed, args):
    count = len(packed)
    first = len(args) == 2
    return call(
        lambda *refs: attend_kernel(first, refs[:count], refs[count:]),
        [mix_shape],
        (*packed, *args),
        attend_flops * count // 2,
        scratch=attend_scratch(KEYS * count // 2),
        limit=24,
    )[0]


def attend_last(args):
    return call(
        attend_last_kernel,
        [jax.ShapeDtypeStruct((HEADS, STATE, OWN_Q), f32)] * 2,
        args,
        attend_flops,
        scratch=attend_scratch(KEYS)
        + [
            pltpu.VMEM((HEADS, SUMS, ALL_Q), f32),
            pltpu.VMEM((HEADS, 8, ALL_Q), f32),
            pltpu.VMEM((2 * SIDE, BLOCK // 2, LANES), bf16),
            pltpu.VMEM((KEYS, ALL_Q), f32),
        ],
        limit=20,
    )


def merge_kernel(stay_ref, came_ref, *send_refs):
    parts = []
    for head in range(HEADS):
        stay = stay_ref[head]
        came = came_ref[head]
        peak = jnp.maximum(stay[HD + 1 : HD + 2], came[HD + 1 : HD + 2])
        fade_stay = jnp.exp2(stay[HD + 1 : HD + 2] - peak)
        fade_came = jnp.exp2(came[HD + 1 : HD + 2] - peak)
        total = stay[HD : HD + 1] * fade_stay + came[HD : HD + 1] * fade_came
        mixed = stay[:HD] * fade_stay + came[:HD] * fade_came
        parts.append(mixed / total)
    turned = jnp.concatenate(parts, axis=0).T
    for peer in range(GROUPS):
        send_refs[peer][...] = pack(turned[peer * ROWS : (peer + 1) * ROWS])


def after_kernel(*refs):
    came_refs = refs[:GROUPS]
    after_ref, wo_ref, up_ref, down_ref, train_ref, test_ref, pieces_ref = refs[GROUPS:]
    for turn in range(GROUPS):
        pieces_ref[own_class() ^ turn] = came_refs[turn][...]
    mixes = [unpack(pieces_ref[index]) for index in range(GROUPS)]
    row_mix = jnp.concatenate(mixes, axis=0).astype(bf16)
    after_row = after_ref[...].reshape(GROUPS * ROWS, E) + mm(row_mix, wo_ref[...])
    third = layer_norm(after_row).astype(bf16)
    raised = mm(third, up_ref[...])
    hidden = (0.5 * raised * (1.0 + lax.erf(raised * (0.5**0.5)))).astype(bf16)
    result = (after_row + mm(hidden, down_ref[...])).astype(bf16)
    for index in range(GROUPS):
        low = index * ROWS
        left = index * E
        train_ref[:, left : left + E] = result[low : low + TRAIN_ROWS]
        test_ref[:, left : left + E] = result[low + TRAIN_ROWS : low + ROWS]


def shift(size, by):
    return [(index, (index + by) % size) for index in range(size)]


def layer(train_cells, test_cells, feat_weights, row_weights, mlp_up, mlp_down):
    swap = [(0, 1), (1, 0)]
    joined = jnp.concatenate([train_cells, test_cells], axis=0)
    other = lax.ppermute(joined, "feat", swap)
    near = call(
        near_kernel,
        [
            jax.ShapeDtypeStruct((GROUPS, ROWS, E), f32),
            jax.ShapeDtypeStruct((GROUPS * ROWS, E), bf16),
            jax.ShapeDtypeStruct((GROUPS, ROWS, 128), f32),
            jax.ShapeDtypeStruct((GROUPS, ROWS, 128), f32),
            jax.ShapeDtypeStruct((GROUPS, ROWS, E), f32),
        ],
        (train_cells, test_cells, feat_weights),
        10**9,
    )
    after_feat, *pieces = call(
        before_kernel,
        [jax.ShapeDtypeStruct((GROUPS, ROWS, E), f32)] + [piece_shape] * GROUPS,
        (other, feat_weights, *near),
        10**9,
        scratch=[pltpu.VMEM((GROUPS, PACK, LANES), bf16)],
    )
    received, keys = call(
        gather_kernel,
        [
            jax.ShapeDtypeStruct((GROUPS, PACK, LANES), bf16),
            jax.ShapeDtypeStruct((GROUPS * TRAIN_PACK, LANES), bf16),
        ],
        exchange(pieces),
        10**6,
        limit=4,
    )
    column = [keys]
    for by in (1, 3, 2):
        column.append(lax.ppermute(keys, "z_hi", shift(SIDE, by)))
    received_other = lax.ppermute(received, "core", swap)
    early = stack(*column[:2])
    early_above = lax.ppermute(early, "x", shift(4, 1))
    early_below = lax.ppermute(early, "x", shift(4, 3))
    folded, value_turned = call(
        fold_kernel,
        [
            jax.ShapeDtypeStruct((HEADS, FOLD, ALL_Q), bf16),
            jax.ShapeDtypeStruct((E, E), bf16),
        ],
        (received, received_other, row_weights),
        10**9,
    )
    column, folded = lax.optimization_barrier((column[2:], folded))
    late = stack(*column)
    late_above = lax.ppermute(late, "x", shift(4, 1))
    late_below = lax.ppermute(late, "x", shift(4, 3))
    mix = attend((early, late), (value_turned, folded))
    mix, early_above, late_below = lax.optimization_barrier((mix, early_above, late_below))
    far_early = lax.ppermute(early_above, "x", shift(4, 1))
    far_late = lax.ppermute(late_below, "x", shift(4, 3))
    middle = (early_above, early_below, late_above, late_below)
    mix = attend(middle, (value_turned, folded, mix))
    packed = (far_early, far_late, early, late) + middle
    stay, leave = attend_last(packed + (value_turned, folded, mix))
    came = lax.ppermute(leave, "core", swap)
    mixed = call(merge_kernel, [piece_shape] * GROUPS, (stay, came), 10**7)
    train_out, test_out = call(
        after_kernel,
        [
            jax.ShapeDtypeStruct((TRAIN_ROWS, GROUPS * E), bf16),
            jax.ShapeDtypeStruct((TEST_ROWS, GROUPS * E), bf16),
        ],
        (*exchange(mixed), after_feat, row_weights[3], mlp_up, mlp_down),
        10**9,
        scratch=[pltpu.VMEM((GROUPS, PACK, LANES), bf16)],
    )
    return (train_out, test_out)


def solution(mesh):
    split = Mesh(
        mesh.devices.reshape(2, 4, 4, 2, 2, 2), ("y_lo", "x", "z_hi", "z_lo", "core", "feat")
    )
    rows = ("y_lo", "x", "z_hi", "z_lo", "core")
    return jax.shard_map(
        layer,
        mesh=split,
        in_specs=(P(rows, "feat"), P(rows, "feat"), P(), P(), P(), P()),
        out_specs=(P(rows, "feat"), P(rows, "feat")),
        check_vma=False,
    )
```

```python
import math

import jax
import jax.numpy as jnp
from jax import lax
from jax.experimental import pallas as pl
from jax.experimental.pallas import tpu as pltpu
from jax.sharding import Mesh
from jax.sharding import PartitionSpec as P

E = 192
HEADS = 6
HD = 32
GROUPS = 4
TRAIN_ROWS = 64
TEST_ROWS = 32
ROWS = TRAIN_ROWS + TEST_ROWS
SIDE = 4
LANES = 128
REST = E - LANES
TRAIN_PACK = TRAIN_ROWS + TRAIN_ROWS // 2
PACK = ROWS + ROWS // 2
OWN_Q = GROUPS * ROWS
ALL_Q = 2 * OWN_Q
SOURCES = GROUPS * SIDE
KEYS = SOURCES * TRAIN_ROWS
SUMS = HD + 16
FOLD = E + 16
PROBES = 16
KEY_STEP = 256
AHEAD = 2
BLOCK = SOURCES * TRAIN_PACK
STATE = HD + 8

eps_norm = 1e-05
far_below = -3e38
safe_size = 2.0**60
log2_scale = HD ** (-0.5) * math.log2(math.e)


bf16 = jnp.bfloat16
f32 = jnp.float32


classes = ("y_lo", "z_lo")
piece_shape = jax.ShapeDtypeStruct((PACK, LANES), bf16)


def mm(left, right):
    return jnp.dot(left, right, preferred_element_type=f32)


def mm_nt(left, right):
    return lax.dot_general(left, right, (((1,), (1,)), ((), ())), preferred_element_type=f32)


def layer_norm(values_in):
    centred = values_in - jnp.mean(values_in, axis=-1, keepdims=True)
    spread = jnp.mean(centred * centred, axis=-1, keepdims=True)
    return centred * lax.rsqrt(spread + eps_norm)


def call(kernel, outs, args, flops, scratch=(), limit=12):
    in_vmem = pl.BlockSpec(memory_space=pltpu.VMEM)
    return pl.pallas_call(
        kernel,
        out_shape=outs,
        in_specs=[in_vmem] * len(args),
        out_specs=[in_vmem] * len(outs),
        scratch_shapes=list(scratch),
        compiler_params=pltpu.CompilerParams(vmem_limit_bytes=limit * 2**20),
        cost_estimate=pl.CostEstimate(flops=flops, transcendentals=0, bytes_accessed=2**20),
    )(*args)


def pack_rows(rows):
    half = rows.shape[0] // 2
    rest = rows[:, LANES:]
    return [rows[:, :LANES], jnp.concatenate([rest[:half], rest[half:]], axis=1)]


def pack(rows):
    parts = pack_rows(rows[:TRAIN_ROWS]) + pack_rows(rows[TRAIN_ROWS:])
    return jnp.concatenate(parts, axis=0).astype(bf16)


def unpack_rows(packed):
    height = packed.shape[0] * 2 // 3
    rest = packed[height:]
    rest = jnp.concatenate([rest[:, :REST], rest[:, REST:]], axis=0)
    return jnp.concatenate([packed[:height], rest], axis=1)


def unpack(packed):
    packed = packed.astype(f32)
    parts = [unpack_rows(packed[:TRAIN_PACK]), unpack_rows(packed[TRAIN_PACK:])]
    return jnp.concatenate(parts, axis=0)


def head_maps():
    head_of = lax.broadcasted_iota(jnp.int32, (E, 128), 0) >> 5
    head_in = lax.broadcasted_iota(jnp.int32, (E, 128), 1)
    head_to = lax.broadcasted_iota(jnp.int32, (128, E), 1) >> 5
    head_out = lax.broadcasted_iota(jnp.int32, (128, E), 0)
    gather = jnp.where(head_of == head_in, 1.0, 0.0).astype(bf16)
    return gather, jnp.where(head_to == head_out, 1.0, 0.0).astype(bf16)


def rows_of(table, index):
    return table[index * ROWS : (index + 1) * ROWS]


def group_scores(asked, keys, gather):
    products = [asked * rows_of(keys, j) for j in range(GROUPS)]
    scores = mm(jnp.concatenate(products, axis=0), gather)
    return [rows_of(scores, j) for j in range(GROUPS)]


def halves(total):
    high = total.astype(bf16)
    return [high, (total - high.astype(f32)).astype(bf16)]


def near_kernel(
    joined_ref,
    weights_ref,
    cells_ref,
    query_ref,
    peak_ref,
    total_ref,
    mixed_ref,
):
    parts = []
    for index in range(GROUPS):
        cell = joined_ref[:, index * E : (index + 1) * E].astype(f32)
        cells_ref[index] = cell
        parts.append(layer_norm(cell).astype(bf16))
    normed = jnp.concatenate(parts, axis=0)
    queries = (mm(normed, weights_ref[0]) * log2_scale).astype(bf16)
    query_ref[...] = queries
    keys = mm(normed, weights_ref[1]).astype(bf16)
    values = mm(normed, weights_ref[2]).astype(bf16).astype(f32)
    gather, spread = head_maps()
    for index in range(GROUPS):
        scores = group_scores(rows_of(queries, index), keys, gather)
        peak = scores[0]
        for one in scores[1:]:
            peak = jnp.maximum(peak, one)
        weights = [jnp.exp2(one - peak) for one in scores]
        total = weights[0]
        for one in weights[1:]:
            total = total + one
        wide = mm(jnp.concatenate([one.astype(bf16) for one in weights], axis=0), spread)
        mixed = rows_of(wide, 0) * rows_of(values, 0)
        for j in range(1, GROUPS):
            mixed = mixed + rows_of(wide, j) * rows_of(values, j)
        peak_ref[index] = peak
        total_ref[index] = total
        mixed_ref[index] = mixed


def own_class():
    return lax.axis_index(classes)


def before_kernel(
    other_ref, weights_ref, cells_ref, query_ref, peak_ref, total_ref, mixed_ref, after_ref, *refs
):
    send_refs, pieces_ref = refs[:GROUPS], refs[GROUPS]
    parts = []
    for index in range(GROUPS):
        cell = other_ref[:, index * E : (index + 1) * E].astype(f32)
        parts.append(layer_norm(cell).astype(bf16))
    normed = jnp.concatenate(parts, axis=0)
    keys = mm(normed, weights_ref[1]).astype(bf16)
    values = mm(normed, weights_ref[2]).astype(bf16).astype(f32)
    gather, spread = head_maps()
    mixtures = []
    for index in range(GROUPS):
        scores = group_scores(query_ref[index * ROWS : (index + 1) * ROWS, :], keys, gather)
        near_peak = peak_ref[index]
        peak = near_peak
        for one in scores:
            peak = jnp.maximum(peak, one)
        fade = jnp.exp2(near_peak - peak)
        weights = [jnp.exp2(one - peak) for one in scores]
        total = total_ref[index] * fade
        for one in weights:
            total = total + one
        widened = [one.astype(bf16) for one in weights] + halves(fade) + halves(total)
        wide = mm(jnp.concatenate(widened, axis=0), spread)
        mixed = mixed_ref[index] * (rows_of(wide, GROUPS) + rows_of(wide, GROUPS + 1))
        for j in range(GROUPS):
            mixed = mixed + rows_of(wide, j) * rows_of(values, j)
        whole = rows_of(wide, GROUPS + 2) + rows_of(wide, GROUPS + 3)
        mixtures.append((mixed / whole).astype(bf16))
    moved = mm(jnp.concatenate(mixtures, axis=0), weights_ref[3]).astype(bf16).astype(f32)
    for index in range(GROUPS):
        after = cells_ref[index] + moved[index * ROWS : (index + 1) * ROWS]
        after_ref[index] = after
        pieces_ref[index] = pack(layer_norm(after))
    for turn in range(GROUPS):
        send_refs[turn][...] = pieces_ref[own_class() ^ turn]


def gather_kernel(*refs):
    received_ref, keys_ref = refs[GROUPS:]
    for turn in range(GROUPS):
        piece = refs[turn][...]
        received_ref[turn] = piece
        keys_ref[turn * TRAIN_PACK : (turn + 1) * TRAIN_PACK, :] = piece[:TRAIN_PACK]


def exchange(pieces):
    came = [pieces[0]]
    for turn in range(1, GROUPS):
        pairs = [(one, one ^ turn) for one in range(GROUPS)]
        came.append(lax.ppermute(pieces[turn], classes, pairs))
    return came


def fold_kernel(own_ref, other_ref, weights_ref, folded_ref, turned_ref):
    turned_ref[...] = weights_ref[2].astype(f32).T.astype(bf16)
    parts = [unpack(one_ref[index]) for one_ref in (own_ref, other_ref) for index in range(GROUPS)]
    asked = jnp.concatenate(parts, axis=0).astype(bf16)
    probes = jnp.concatenate([parts[0][:PROBES], parts[GROUPS][:PROBES]], axis=0).astype(bf16)
    turned = weights_ref[0].astype(f32).T.astype(bf16)
    queries = (mm_nt(turned, asked) * log2_scale).astype(bf16)
    weight = weights_ref[1].astype(f32)
    probed = mm(probes, weights_ref[1])
    head_of = lax.broadcasted_iota(jnp.int32, (1, E), 1) >> 5
    masks = [jnp.where(head_of == head, 1.0, 0.0) for head in range(HEADS)]
    stacked = [weight * mask for mask in masks] + [probed * mask for mask in masks]
    folded = mm(jnp.concatenate(stacked, axis=0).astype(bf16), queries)
    row = lax.broadcasted_iota(jnp.int32, (FOLD - E, ALL_Q), 0)
    for head in range(HEADS):
        folded_ref[head, :E, :] = folded[head * E : (head + 1) * E].astype(bf16)
        low = HEADS * E + head * 2 * PROBES
        peak = jnp.max(folded[low : low + 2 * PROBES], axis=0, keepdims=True)
        folded_ref[head, E:, :] = jnp.where(row == 0, -peak, 0.0).astype(bf16)


def stack_kernel(upper_ref, lower_ref, both_ref):
    both_ref[: BLOCK // 4, :] = upper_ref[...]
    both_ref[BLOCK // 4 :, :] = lower_ref[...]


def stack(upper, lower):
    return call(
        stack_kernel,
        [jax.ShapeDtypeStruct((BLOCK // 2, LANES), bf16)],
        (upper, lower),
        10**6,
        limit=4,
    )[0]


def unpack_keys(packed_refs, keys_ref):
    half = TRAIN_ROWS // 2
    each = SOURCES // 2
    for source in range(len(packed_refs) * each):
        packed_ref = packed_refs[source // each]
        low = source * TRAIN_ROWS
        top = source % each * TRAIN_PACK
        rest = packed_ref[top + TRAIN_ROWS : top + TRAIN_PACK, :]
        keys_ref[low : low + TRAIN_ROWS, :LANES] = packed_ref[top : top + TRAIN_ROWS, :]
        keys_ref[low : low + half, LANES:E] = rest[:, :REST]
        keys_ref[low + half : low + TRAIN_ROWS, LANES:E] = rest[:, REST:]
    keys_ref[:, E:] = jnp.ones((keys_ref.shape[0], FOLD - E), bf16)


def turn_values(wv_ref, keys_ref, values_ref):
    values = mm_nt(wv_ref[...], keys_ref[:, :E]).astype(bf16)
    for head in range(HEADS):
        values_ref[head, 0:HD, :] = values[head * HD : (head + 1) * HD, :]
        values_ref[head, HD:SUMS, :] = jnp.ones((SUMS - HD, keys_ref.shape[0]), bf16)


def attend_heads(packed_refs, wv_ref, folded_ref, keys_ref, values_ref, finish):
    unpack_keys(packed_refs, keys_ref)
    turn_values(wv_ref, keys_ref, values_ref)
    steps = keys_ref.shape[0] // KEY_STEP
    waiting = []
    sums = {}

    def drain():
        head, step, weights = waiting.pop(0)
        part = mm(values_ref[head, :, step * KEY_STEP : (step + 1) * KEY_STEP], weights)
        sums[head] = sums[head] + part if step else part
        if step == steps - 1:
            finish(head, sums.pop(head))

    for head in range(HEADS):
        for step in range(steps):
            scores = mm(keys_ref[step * KEY_STEP : (step + 1) * KEY_STEP, :], folded_ref[head])
            waiting.append((head, step, jnp.exp2(scores).astype(bf16)))
            if len(waiting) > AHEAD:
                drain()
    while waiting:
        drain()


def attend_kernel(first, packed_refs, refs):
    wv_ref, folded_ref = refs[:2]
    mix_out, keys_ref, values_ref = refs[-3:]

    def finish(head, mixed):
        mix_out[head] = mixed if first else mixed + refs[2][head]

    attend_heads(packed_refs, wv_ref, folded_ref, keys_ref, values_ref, finish)


def attend_last_kernel(*refs):
    packed_refs = refs[: 2 * SIDE]
    wv_ref, folded_ref, mix_ref, stay_ref, leave_ref = refs[2 * SIDE : 2 * SIDE + 5]
    keys_ref, values_ref, total_ref, peak_ref, blocks_ref, scores_ref = refs[2 * SIDE + 5 :]
    over = [jnp.zeros((8, ALL_Q), f32)]

    def leave(head, total, peak):
        joined = jnp.concatenate([total[: HD + 1], peak, total[HD + 2 : STATE]], axis=0)
        stay_ref[head] = joined[:, :OWN_Q]
        leave_ref[head] = joined[:, OWN_Q:]

    def finish(head, mixed):
        total = mixed + mix_ref[head]
        grown = jnp.where(jnp.abs(total) < safe_size, 0.0, 1.0)
        over[0] = jnp.maximum(over[0], jnp.max(grown.reshape(SUMS // 8, 8, ALL_Q), axis=0))
        leave(head, total, -folded_ref[head, E:, :].astype(f32)[:1])

    attend_heads(packed_refs[:2], wv_ref, folded_ref, keys_ref, values_ref, finish)

    @pl.when(jnp.max(over[0]) > 0.0)
    def _():
        for index, one_ref in enumerate(packed_refs):
            blocks_ref[index] = one_ref[...]
        peak_ref[...] = jnp.full(peak_ref.shape, far_below, f32)
        total_ref[...] = jnp.zeros(total_ref.shape, f32)

        def one_block(index, carry):
            unpack_keys((blocks_ref.at[2 * index], blocks_ref.at[2 * index + 1]), keys_ref)
            turn_values(wv_ref, keys_ref, values_ref)

            def work(head, kept):
                scores_ref[...] = mm(keys_ref[:, :E], folded_ref[head, :E, :])
                old = peak_ref[head][0:1, :]
                peak = jnp.maximum(jnp.max(scores_ref[...], axis=0, keepdims=True), old)
                weights = jnp.exp2(scores_ref[...] - peak).astype(bf16)
                mixed = mm(values_ref[head], weights)
                total_ref[head] = total_ref[head] * jnp.exp2(old - peak) + mixed
                peak_ref[head] = jnp.broadcast_to(peak, (8, ALL_Q))
                return kept

            lax.fori_loop(0, HEADS, work, 0)
            return carry

        lax.fori_loop(0, SIDE, one_block, 0)
        for head in range(HEADS):
            leave(head, total_ref[head], peak_ref[head][0:1, :])


mix_shape = jax.ShapeDtypeStruct((HEADS, SUMS, ALL_Q), f32)
attend_flops = 4 * HEADS * KEYS * ALL_Q * E


def attend_scratch(keys):
    return [pltpu.VMEM((keys, FOLD), bf16), pltpu.VMEM((HEADS, SUMS, keys), bf16)]


def attend(packed, args):
    count = len(packed)
    first = len(args) == 2
    return call(
        lambda *refs: attend_kernel(first, refs[:count], refs[count:]),
        [mix_shape],
        (*packed, *args),
        attend_flops * count // 2,
        scratch=attend_scratch(KEYS * count // 2),
        limit=24,
    )[0]


def attend_last(args):
    return call(
        attend_last_kernel,
        [jax.ShapeDtypeStruct((HEADS, STATE, OWN_Q), f32)] * 2,
        args,
        attend_flops,
        scratch=attend_scratch(KEYS)
        + [
            pltpu.VMEM((HEADS, SUMS, ALL_Q), f32),
            pltpu.VMEM((HEADS, 8, ALL_Q), f32),
            pltpu.VMEM((2 * SIDE, BLOCK // 2, LANES), bf16),
            pltpu.VMEM((KEYS, ALL_Q), f32),
        ],
        limit=20,
    )


def merge_kernel(stay_ref, came_ref, *send_refs):
    parts = []
    for head in range(HEADS):
        stay = stay_ref[head]
        came = came_ref[head]
        peak = jnp.maximum(stay[HD + 1 : HD + 2], came[HD + 1 : HD + 2])
        fade_stay = jnp.exp2(stay[HD + 1 : HD + 2] - peak)
        fade_came = jnp.exp2(came[HD + 1 : HD + 2] - peak)
        total = stay[HD : HD + 1] * fade_stay + came[HD : HD + 1] * fade_came
        mixed = stay[:HD] * fade_stay + came[:HD] * fade_came
        parts.append(mixed / total)
    turned = jnp.concatenate(parts, axis=0).T
    for peer in range(GROUPS):
        send_refs[peer][...] = pack(turned[peer * ROWS : (peer + 1) * ROWS])


def after_kernel(*refs):
    came_refs = refs[:GROUPS]
    after_ref, wo_ref, up_ref, down_ref, train_ref, test_ref, pieces_ref = refs[GROUPS:]
    for turn in range(GROUPS):
        pieces_ref[own_class() ^ turn] = came_refs[turn][...]
    mixes = [unpack(pieces_ref[index]) for index in range(GROUPS)]
    row_mix = jnp.concatenate(mixes, axis=0).astype(bf16)
    after_row = after_ref[...].reshape(GROUPS * ROWS, E) + mm(row_mix, wo_ref[...])
    third = layer_norm(after_row).astype(bf16)
    raised = mm(third, up_ref[...])
    hidden = (0.5 * raised * (1.0 + lax.erf(raised * (0.5**0.5)))).astype(bf16)
    result = (after_row + mm(hidden, down_ref[...])).astype(bf16)
    for index in range(GROUPS):
        low = index * ROWS
        left = index * E
        train_ref[:, left : left + E] = result[low : low + TRAIN_ROWS]
        test_ref[:, left : left + E] = result[low + TRAIN_ROWS : low + ROWS]


def shift(size, by):
    return [(index, (index + by) % size) for index in range(size)]


def layer(train_cells, test_cells, feat_weights, row_weights, mlp_up, mlp_down):
    swap = [(0, 1), (1, 0)]
    low = jnp.array(-jnp.inf, bf16)
    upper = lax.pad(train_cells, low, ((0, TEST_ROWS, 0), (0, 0, 0)))
    joined = jnp.maximum(upper, lax.pad(test_cells, low, ((TRAIN_ROWS, 0, 0), (0, 0, 0))))
    other = lax.ppermute(joined, "feat", swap)
    near = call(
        near_kernel,
        [
            jax.ShapeDtypeStruct((GROUPS, ROWS, E), f32),
            jax.ShapeDtypeStruct((GROUPS * ROWS, E), bf16),
            jax.ShapeDtypeStruct((GROUPS, ROWS, 128), f32),
            jax.ShapeDtypeStruct((GROUPS, ROWS, 128), f32),
            jax.ShapeDtypeStruct((GROUPS, ROWS, E), f32),
        ],
        (joined, feat_weights),
        10**9,
    )
    after_feat, *pieces = call(
        before_kernel,
        [jax.ShapeDtypeStruct((GROUPS, ROWS, E), f32)] + [piece_shape] * GROUPS,
        (other, feat_weights, *near),
        10**9,
        scratch=[pltpu.VMEM((GROUPS, PACK, LANES), bf16)],
    )
    received, keys = call(
        gather_kernel,
        [
            jax.ShapeDtypeStruct((GROUPS, PACK, LANES), bf16),
            jax.ShapeDtypeStruct((GROUPS * TRAIN_PACK, LANES), bf16),
        ],
        exchange(pieces),
        10**6,
        limit=4,
    )
    column = [keys]
    for by in (1, 3, 2):
        column.append(lax.ppermute(keys, "z_hi", shift(SIDE, by)))
    received_other = lax.ppermute(received, "core", swap)
    early = stack(*column[:2])
    early_above = lax.ppermute(early, "x", shift(4, 1))
    early_below = lax.ppermute(early, "x", shift(4, 3))
    folded, value_turned = call(
        fold_kernel,
        [
            jax.ShapeDtypeStruct((HEADS, FOLD, ALL_Q), bf16),
            jax.ShapeDtypeStruct((E, E), bf16),
        ],
        (received, received_other, row_weights),
        10**9,
    )
    column, folded = lax.optimization_barrier((column[2:], folded))
    late = stack(*column)
    late_above = lax.ppermute(late, "x", shift(4, 1))
    late_below = lax.ppermute(late, "x", shift(4, 3))
    mix = attend((early, late), (value_turned, folded))
    mix, early_above = lax.optimization_barrier((mix, early_above))
    mix, late_below = lax.optimization_barrier((mix, late_below))
    far_early = lax.ppermute(early_above, "x", shift(4, 1))
    far_late = lax.ppermute(late_below, "x", shift(4, 3))
    middle = (early_above, early_below, late_above, late_below)
    mix = attend(middle, (value_turned, folded, mix))
    packed = (far_early, far_late, early, late) + middle
    stay, leave = attend_last(packed + (value_turned, folded, mix))
    came = lax.ppermute(leave, "core", swap)
    mixed = call(merge_kernel, [piece_shape] * GROUPS, (stay, came), 10**7)
    train_out, test_out = call(
        after_kernel,
        [
            jax.ShapeDtypeStruct((TRAIN_ROWS, GROUPS * E), bf16),
            jax.ShapeDtypeStruct((TEST_ROWS, GROUPS * E), bf16),
        ],
        (*exchange(mixed), after_feat, row_weights[3], mlp_up, mlp_down),
        10**9,
        scratch=[pltpu.VMEM((GROUPS, PACK, LANES), bf16)],
    )
    return (train_out, test_out)


def solution(mesh):
    split = Mesh(
        mesh.devices.reshape(2, 4, 4, 2, 2, 2), ("y_lo", "x", "z_hi", "z_lo", "core", "feat")
    )
    rows = ("y_lo", "x", "z_hi", "z_lo", "core")
    return jax.shard_map(
        layer,
        mesh=split,
        in_specs=(P(rows, "feat"), P(rows, "feat"), P(), P(), P(), P()),
        out_specs=(P(rows, "feat"), P(rows, "feat")),
        check_vma=False,
    )
```

```python
import math

import jax
import jax.numpy as jnp
from jax import lax
from jax.experimental import pallas as pl
from jax.experimental.pallas import tpu as pltpu
from jax.sharding import Mesh
from jax.sharding import PartitionSpec as P

E = 192
HEADS = 6
HD = 32
GROUPS = 4
TRAIN_ROWS = 64
TEST_ROWS = 32
ROWS = TRAIN_ROWS + TEST_ROWS
SIDE = 4
LANES = 128
REST = E - LANES
TRAIN_PACK = TRAIN_ROWS + TRAIN_ROWS // 2
PACK = ROWS + ROWS // 2
OWN_Q = GROUPS * ROWS
ALL_Q = 2 * OWN_Q
SOURCES = GROUPS * SIDE
KEYS = SOURCES * TRAIN_ROWS
SUMS = HD + 16
FOLD = E + 16
PROBES = 16
KEY_STEP = 256
AHEAD = 2
BLOCK = SOURCES * TRAIN_PACK
STATE = HD + 8

eps_norm = 1e-05
far_below = -3e38
safe_size = 2.0**60
log2_scale = HD ** (-0.5) * math.log2(math.e)


bf16 = jnp.bfloat16
f32 = jnp.float32


classes = ("y_lo", "z_lo")
piece_shape = jax.ShapeDtypeStruct((PACK, LANES), bf16)


def mm(left, right):
    return jnp.dot(left, right, preferred_element_type=f32)


def mm_nt(left, right):
    return lax.dot_general(left, right, (((1,), (1,)), ((), ())), preferred_element_type=f32)


def layer_norm(values_in):
    centred = values_in - jnp.mean(values_in, axis=-1, keepdims=True)
    spread = jnp.mean(centred * centred, axis=-1, keepdims=True)
    return centred * lax.rsqrt(spread + eps_norm)


def call(kernel, outs, args, flops, scratch=(), limit=12):
    in_vmem = pl.BlockSpec(memory_space=pltpu.VMEM)
    return pl.pallas_call(
        kernel,
        out_shape=outs,
        in_specs=[in_vmem] * len(args),
        out_specs=[in_vmem] * len(outs),
        scratch_shapes=list(scratch),
        compiler_params=pltpu.CompilerParams(vmem_limit_bytes=limit * 2**20),
        cost_estimate=pl.CostEstimate(flops=flops, transcendentals=0, bytes_accessed=2**20),
    )(*args)


def pack_rows(rows):
    half = rows.shape[0] // 2
    rest = rows[:, LANES:]
    return [rows[:, :LANES], jnp.concatenate([rest[:half], rest[half:]], axis=1)]


def pack(rows):
    parts = pack_rows(rows[:TRAIN_ROWS]) + pack_rows(rows[TRAIN_ROWS:])
    return jnp.concatenate(parts, axis=0).astype(bf16)


def unpack_rows(packed):
    height = packed.shape[0] * 2 // 3
    rest = packed[height:]
    rest = jnp.concatenate([rest[:, :REST], rest[:, REST:]], axis=0)
    return jnp.concatenate([packed[:height], rest], axis=1)


def unpack(packed):
    packed = packed.astype(f32)
    parts = [unpack_rows(packed[:TRAIN_PACK]), unpack_rows(packed[TRAIN_PACK:])]
    return jnp.concatenate(parts, axis=0)


def head_maps():
    head_of = lax.broadcasted_iota(jnp.int32, (E, 128), 0) >> 5
    head_in = lax.broadcasted_iota(jnp.int32, (E, 128), 1)
    head_to = lax.broadcasted_iota(jnp.int32, (128, E), 1) >> 5
    head_out = lax.broadcasted_iota(jnp.int32, (128, E), 0)
    gather = jnp.where(head_of == head_in, 1.0, 0.0).astype(bf16)
    return gather, jnp.where(head_to == head_out, 1.0, 0.0).astype(bf16)


def rows_of(table, index):
    return table[index * ROWS : (index + 1) * ROWS]


def group_scores(asked, keys, gather):
    products = [asked * rows_of(keys, j) for j in range(GROUPS)]
    scores = mm(jnp.concatenate(products, axis=0), gather)
    return [rows_of(scores, j) for j in range(GROUPS)]


def halves(total):
    high = total.astype(bf16)
    return [high, (total - high.astype(f32)).astype(bf16)]


def near_kernel(
    joined_ref,
    weights_ref,
    cells_ref,
    query_ref,
    peak_ref,
    total_ref,
    mixed_ref,
):
    parts = []
    for index in range(GROUPS):
        cell = joined_ref[:, index * E : (index + 1) * E].astype(f32)
        cells_ref[index] = cell
        parts.append(layer_norm(cell).astype(bf16))
    normed = jnp.concatenate(parts, axis=0)
    queries = (mm(normed, weights_ref[0]) * log2_scale).astype(bf16)
    query_ref[...] = queries
    keys = mm(normed, weights_ref[1]).astype(bf16)
    values = mm(normed, weights_ref[2]).astype(bf16).astype(f32)
    gather, spread = head_maps()
    for index in range(GROUPS):
        scores = group_scores(rows_of(queries, index), keys, gather)
        peak = scores[0]
        for one in scores[1:]:
            peak = jnp.maximum(peak, one)
        weights = [jnp.exp2(one - peak) for one in scores]
        total = weights[0]
        for one in weights[1:]:
            total = total + one
        wide = mm(jnp.concatenate([one.astype(bf16) for one in weights], axis=0), spread)
        mixed = rows_of(wide, 0) * rows_of(values, 0)
        for j in range(1, GROUPS):
            mixed = mixed + rows_of(wide, j) * rows_of(values, j)
        peak_ref[index] = peak
        total_ref[index] = total
        mixed_ref[index] = mixed


def own_class():
    return lax.axis_index(classes)


def before_kernel(
    other_ref, weights_ref, cells_ref, query_ref, peak_ref, total_ref, mixed_ref, after_ref, *refs
):
    send_refs, pieces_ref = refs[:GROUPS], refs[GROUPS]
    parts = []
    for index in range(GROUPS):
        cell = other_ref[:, index * E : (index + 1) * E].astype(f32)
        parts.append(layer_norm(cell).astype(bf16))
    normed = jnp.concatenate(parts, axis=0)
    keys = mm(normed, weights_ref[1]).astype(bf16)
    values = mm(normed, weights_ref[2]).astype(bf16).astype(f32)
    gather, spread = head_maps()
    mixtures = []
    for index in range(GROUPS):
        scores = group_scores(query_ref[index * ROWS : (index + 1) * ROWS, :], keys, gather)
        near_peak = peak_ref[index]
        peak = near_peak
        for one in scores:
            peak = jnp.maximum(peak, one)
        fade = jnp.exp2(near_peak - peak)
        weights = [jnp.exp2(one - peak) for one in scores]
        total = total_ref[index] * fade
        for one in weights:
            total = total + one
        widened = [one.astype(bf16) for one in weights] + halves(fade) + halves(total)
        wide = mm(jnp.concatenate(widened, axis=0), spread)
        mixed = mixed_ref[index] * (rows_of(wide, GROUPS) + rows_of(wide, GROUPS + 1))
        for j in range(GROUPS):
            mixed = mixed + rows_of(wide, j) * rows_of(values, j)
        whole = rows_of(wide, GROUPS + 2) + rows_of(wide, GROUPS + 3)
        mixtures.append((mixed / whole).astype(bf16))
    moved = mm(jnp.concatenate(mixtures, axis=0), weights_ref[3]).astype(bf16).astype(f32)
    for index in range(GROUPS):
        after = cells_ref[index] + moved[index * ROWS : (index + 1) * ROWS]
        after_ref[index] = after
        pieces_ref[index] = pack(layer_norm(after))
    for turn in range(GROUPS):
        send_refs[turn][...] = pieces_ref[own_class() ^ turn]


def gather_kernel(*refs):
    received_ref, keys_ref = refs[GROUPS:]
    for turn in range(GROUPS):
        piece = refs[turn][...]
        received_ref[turn] = piece
        keys_ref[turn * TRAIN_PACK : (turn + 1) * TRAIN_PACK, :] = piece[:TRAIN_PACK]


def exchange(pieces):
    came = [pieces[0]]
    for turn in range(1, GROUPS):
        pairs = [(one, one ^ turn) for one in range(GROUPS)]
        came.append(lax.ppermute(pieces[turn], classes, pairs))
    return came


def fold_kernel(own_ref, other_ref, weights_ref, folded_ref, turned_ref):
    turned_ref[...] = weights_ref[2].astype(f32).T.astype(bf16)
    parts = [unpack(one_ref[index]) for one_ref in (own_ref, other_ref) for index in range(GROUPS)]
    asked = jnp.concatenate(parts, axis=0).astype(bf16)
    probes = jnp.concatenate([parts[0][:PROBES], parts[GROUPS][:PROBES]], axis=0).astype(bf16)
    turned = weights_ref[0].astype(f32).T.astype(bf16)
    queries = (mm_nt(turned, asked) * log2_scale).astype(bf16)
    weight = weights_ref[1].astype(f32)
    probed = mm(probes, weights_ref[1])
    head_of = lax.broadcasted_iota(jnp.int32, (1, E), 1) >> 5
    masks = [jnp.where(head_of == head, 1.0, 0.0) for head in range(HEADS)]
    stacked = [weight * mask for mask in masks] + [probed * mask for mask in masks]
    folded = mm(jnp.concatenate(stacked, axis=0).astype(bf16), queries)
    row = lax.broadcasted_iota(jnp.int32, (FOLD - E, ALL_Q), 0)
    for head in range(HEADS):
        folded_ref[head, :E, :] = folded[head * E : (head + 1) * E].astype(bf16)
        low = HEADS * E + head * 2 * PROBES
        peak = jnp.max(folded[low : low + 2 * PROBES], axis=0, keepdims=True)
        folded_ref[head, E:, :] = jnp.where(row == 0, -peak, 0.0).astype(bf16)


def stack_kernel(upper_ref, lower_ref, both_ref):
    both_ref[: BLOCK // 4, :] = upper_ref[...]
    both_ref[BLOCK // 4 :, :] = lower_ref[...]


def choose_kernel(early_above, early_below, late_above, late_below, chosen_ref):
    core = lax.axis_index("core")
    for turn, parts in enumerate(((early_above, late_above), (early_below, late_below))):

        @pl.when(core == turn)
        def _():
            chosen_ref[: BLOCK // 2, :] = parts[0][...]
            chosen_ref[BLOCK // 2 :, :] = parts[1][...]


def stack(upper, lower):
    return call(
        stack_kernel,
        [jax.ShapeDtypeStruct((BLOCK // 2, LANES), bf16)],
        (upper, lower),
        10**6,
        limit=4,
    )[0]


def unpack_keys(packed_refs, keys_ref):
    half = TRAIN_ROWS // 2
    each = SOURCES // 2
    for source in range(len(packed_refs) * each):
        packed_ref = packed_refs[source // each]
        low = source * TRAIN_ROWS
        top = source % each * TRAIN_PACK
        rest = packed_ref[top + TRAIN_ROWS : top + TRAIN_PACK, :]
        keys_ref[low : low + TRAIN_ROWS, :LANES] = packed_ref[top : top + TRAIN_ROWS, :]
        keys_ref[low : low + half, LANES:E] = rest[:, :REST]
        keys_ref[low + half : low + TRAIN_ROWS, LANES:E] = rest[:, REST:]
    keys_ref[:, E:] = jnp.ones((keys_ref.shape[0], FOLD - E), bf16)


def turn_values(wv_ref, keys_ref, values_ref):
    values = mm_nt(wv_ref[...], keys_ref[:, :E]).astype(bf16)
    for head in range(HEADS):
        values_ref[head, 0:HD, :] = values[head * HD : (head + 1) * HD, :]
        values_ref[head, HD:SUMS, :] = jnp.ones((SUMS - HD, keys_ref.shape[0]), bf16)


def attend_heads(packed_refs, wv_ref, folded_ref, keys_ref, values_ref, finish):
    unpack_keys(packed_refs, keys_ref)
    turn_values(wv_ref, keys_ref, values_ref)
    steps = keys_ref.shape[0] // KEY_STEP
    waiting = []
    sums = {}

    def drain():
        head, step, weights = waiting.pop(0)
        part = mm(values_ref[head, :, step * KEY_STEP : (step + 1) * KEY_STEP], weights)
        sums[head] = sums[head] + part if step else part
        if step == steps - 1:
            finish(head, sums.pop(head))

    for head in range(HEADS):
        for step in range(steps):
            scores = mm(keys_ref[step * KEY_STEP : (step + 1) * KEY_STEP, :], folded_ref[head])
            waiting.append((head, step, jnp.exp2(scores).astype(bf16)))
            if len(waiting) > AHEAD:
                drain()
    while waiting:
        drain()


def attend_kernel(first, packed_refs, refs):
    wv_ref, folded_ref = refs[:2]
    mix_out, keys_ref, values_ref = refs[-3:]

    def finish(head, mixed):
        mix_out[head] = mixed if first else mixed + refs[2][head]

    attend_heads(packed_refs, wv_ref, folded_ref, keys_ref, values_ref, finish)


def attend_last_kernel(*refs):
    far_ref = refs[0]
    packed_refs = (far_ref.at[: BLOCK // 2], far_ref.at[BLOCK // 2 :]) + refs[1 : 2 * SIDE - 1]
    wv_ref, folded_ref, mix_ref, stay_ref, leave_ref = refs[2 * SIDE - 1 : 2 * SIDE + 4]
    keys_ref, values_ref, total_ref, peak_ref, blocks_ref, scores_ref = refs[2 * SIDE + 4 :]
    over = [jnp.zeros((8, ALL_Q), f32)]

    def leave(head, total, peak):
        joined = jnp.concatenate([total[: HD + 1], peak, total[HD + 2 : STATE]], axis=0)
        stay_ref[head] = joined[:, :OWN_Q]
        leave_ref[head] = joined[:, OWN_Q:]

    def finish(head, mixed):
        total = mixed + mix_ref[head]
        grown = jnp.where(jnp.abs(total) < safe_size, 0.0, 1.0)
        over[0] = jnp.maximum(over[0], jnp.max(grown.reshape(SUMS // 8, 8, ALL_Q), axis=0))
        leave(head, total, -folded_ref[head, E:, :].astype(f32)[:1])

    attend_heads(packed_refs[:2], wv_ref, folded_ref, keys_ref, values_ref, finish)

    @pl.when(jnp.max(over[0]) > 0.0)
    def _():
        for index, one_ref in enumerate(packed_refs):
            blocks_ref[index] = one_ref[...]
        peak_ref[...] = jnp.full(peak_ref.shape, far_below, f32)
        total_ref[...] = jnp.zeros(total_ref.shape, f32)

        def one_block(index, carry):
            unpack_keys((blocks_ref.at[2 * index], blocks_ref.at[2 * index + 1]), keys_ref)
            turn_values(wv_ref, keys_ref, values_ref)

            def work(head, kept):
                scores_ref[...] = mm(keys_ref[:, :E], folded_ref[head, :E, :])
                old = peak_ref[head][0:1, :]
                peak = jnp.maximum(jnp.max(scores_ref[...], axis=0, keepdims=True), old)
                weights = jnp.exp2(scores_ref[...] - peak).astype(bf16)
                mixed = mm(values_ref[head], weights)
                total_ref[head] = total_ref[head] * jnp.exp2(old - peak) + mixed
                peak_ref[head] = jnp.broadcast_to(peak, (8, ALL_Q))
                return kept

            lax.fori_loop(0, HEADS, work, 0)
            return carry

        lax.fori_loop(0, SIDE, one_block, 0)
        for head in range(HEADS):
            leave(head, total_ref[head], peak_ref[head][0:1, :])


mix_shape = jax.ShapeDtypeStruct((HEADS, SUMS, ALL_Q), f32)
attend_flops = 4 * HEADS * KEYS * ALL_Q * E


def attend_scratch(keys):
    return [pltpu.VMEM((keys, FOLD), bf16), pltpu.VMEM((HEADS, SUMS, keys), bf16)]


def attend(packed, args):
    count = len(packed)
    first = len(args) == 2
    return call(
        lambda *refs: attend_kernel(first, refs[:count], refs[count:]),
        [mix_shape],
        (*packed, *args),
        attend_flops * count // 2,
        scratch=attend_scratch(KEYS * count // 2),
        limit=24,
    )[0]


def attend_last(args):
    return call(
        attend_last_kernel,
        [jax.ShapeDtypeStruct((HEADS, STATE, OWN_Q), f32)] * 2,
        args,
        attend_flops,
        scratch=attend_scratch(KEYS)
        + [
            pltpu.VMEM((HEADS, SUMS, ALL_Q), f32),
            pltpu.VMEM((HEADS, 8, ALL_Q), f32),
            pltpu.VMEM((2 * SIDE, BLOCK // 2, LANES), bf16),
            pltpu.VMEM((KEYS, ALL_Q), f32),
        ],
        limit=20,
    )


def merge_kernel(stay_ref, came_ref, *send_refs):
    parts = []
    for head in range(HEADS):
        stay = stay_ref[head]
        came = came_ref[head]
        peak = jnp.maximum(stay[HD + 1 : HD + 2], came[HD + 1 : HD + 2])
        fade_stay = jnp.exp2(stay[HD + 1 : HD + 2] - peak)
        fade_came = jnp.exp2(came[HD + 1 : HD + 2] - peak)
        total = stay[HD : HD + 1] * fade_stay + came[HD : HD + 1] * fade_came
        mixed = stay[:HD] * fade_stay + came[:HD] * fade_came
        parts.append(mixed / total)
    turned = jnp.concatenate(parts, axis=0).T
    for peer in range(GROUPS):
        send_refs[peer][...] = pack(turned[peer * ROWS : (peer + 1) * ROWS])


def after_kernel(*refs):
    came_refs = refs[:GROUPS]
    after_ref, wo_ref, up_ref, down_ref, train_ref, test_ref, pieces_ref = refs[GROUPS:]
    for turn in range(GROUPS):
        pieces_ref[own_class() ^ turn] = came_refs[turn][...]
    mixes = [unpack(pieces_ref[index]) for index in range(GROUPS)]
    row_mix = jnp.concatenate(mixes, axis=0).astype(bf16)
    after_row = after_ref[...].reshape(GROUPS * ROWS, E) + mm(row_mix, wo_ref[...])
    third = layer_norm(after_row).astype(bf16)
    raised = mm(third, up_ref[...])
    hidden = (0.5 * raised * (1.0 + lax.erf(raised * (0.5**0.5)))).astype(bf16)
    result = (after_row + mm(hidden, down_ref[...])).astype(bf16)
    for index in range(GROUPS):
        low = index * ROWS
        left = index * E
        train_ref[:, left : left + E] = result[low : low + TRAIN_ROWS]
        test_ref[:, left : left + E] = result[low + TRAIN_ROWS : low + ROWS]


def shift(size, by):
    return [(index, (index + by) % size) for index in range(size)]


def layer(train_cells, test_cells, feat_weights, row_weights, mlp_up, mlp_down):
    swap = [(0, 1), (1, 0)]
    low = jnp.array(-jnp.inf, bf16)
    upper = lax.pad(train_cells, low, ((0, TEST_ROWS, 0), (0, 0, 0)))
    joined = jnp.maximum(upper, lax.pad(test_cells, low, ((TRAIN_ROWS, 0, 0), (0, 0, 0))))
    other = lax.ppermute(joined, "feat", swap)
    near = call(
        near_kernel,
        [
            jax.ShapeDtypeStruct((GROUPS, ROWS, E), f32),
            jax.ShapeDtypeStruct((GROUPS * ROWS, E), bf16),
            jax.ShapeDtypeStruct((GROUPS, ROWS, 128), f32),
            jax.ShapeDtypeStruct((GROUPS, ROWS, 128), f32),
            jax.ShapeDtypeStruct((GROUPS, ROWS, E), f32),
        ],
        (joined, feat_weights),
        10**9,
    )
    after_feat, *pieces = call(
        before_kernel,
        [jax.ShapeDtypeStruct((GROUPS, ROWS, E), f32)] + [piece_shape] * GROUPS,
        (other, feat_weights, *near),
        10**9,
        scratch=[pltpu.VMEM((GROUPS, PACK, LANES), bf16)],
    )
    received, keys = call(
        gather_kernel,
        [
            jax.ShapeDtypeStruct((GROUPS, PACK, LANES), bf16),
            jax.ShapeDtypeStruct((GROUPS * TRAIN_PACK, LANES), bf16),
        ],
        exchange(pieces),
        10**6,
        limit=4,
    )
    column = [keys]
    for by in (1, 3, 2):
        column.append(lax.ppermute(keys, "z_hi", shift(SIDE, by)))
    received_other = lax.ppermute(received, "core", swap)
    early = stack(*column[:2])
    early_above = lax.ppermute(early, "x", shift(4, 1))
    early_below = lax.ppermute(early, "x", shift(4, 3))
    folded, value_turned = call(
        fold_kernel,
        [
            jax.ShapeDtypeStruct((HEADS, FOLD, ALL_Q), bf16),
            jax.ShapeDtypeStruct((E, E), bf16),
        ],
        (received, received_other, row_weights),
        10**9,
    )
    late = stack(*column[2:])
    late_above = lax.ppermute(late, "x", shift(4, 1))
    late_below = lax.ppermute(late, "x", shift(4, 3))
    mix = attend((early, late), (value_turned, folded))
    middle = (early_above, early_below, late_above, late_below)
    mix, middle = lax.optimization_barrier((mix, middle))
    chosen = call(
        choose_kernel, [jax.ShapeDtypeStruct((BLOCK, LANES), bf16)], middle, 10**6, limit=4
    )[0]
    pairs = [(2 * one, (2 * one + 2) % 8) for one in range(4)]
    pairs += [(2 * one + 1, (2 * one + 7) % 8) for one in range(4)]
    far = lax.ppermute(chosen, ("x", "core"), pairs)
    mix = attend(middle, (value_turned, folded, mix))
    packed = (far, early, late) + middle
    stay, leave = attend_last(packed + (value_turned, folded, mix))
    came = lax.ppermute(leave, "core", swap)
    mixed = call(merge_kernel, [piece_shape] * GROUPS, (stay, came), 10**7)
    train_out, test_out = call(
        after_kernel,
        [
            jax.ShapeDtypeStruct((TRAIN_ROWS, GROUPS * E), bf16),
            jax.ShapeDtypeStruct((TEST_ROWS, GROUPS * E), bf16),
        ],
        (*exchange(mixed), after_feat, row_weights[3], mlp_up, mlp_down),
        10**9,
        scratch=[pltpu.VMEM((GROUPS, PACK, LANES), bf16)],
    )
    return (train_out, test_out)


def solution(mesh):
    split = Mesh(
        mesh.devices.reshape(2, 4, 4, 2, 2, 2), ("y_lo", "x", "z_hi", "z_lo", "core", "feat")
    )
    rows = ("y_lo", "x", "z_hi", "z_lo", "core")
    return jax.shard_map(
        layer,
        mesh=split,
        in_specs=(P(rows, "feat"), P(rows, "feat"), P(), P(), P(), P()),
        out_specs=(P(rows, "feat"), P(rows, "feat")),
        check_vma=False,
    )
```
